8 devices in a mesh: ty: 2 (over z, y), tx: 4 (over x, core).
Axes of the slice: x: 2, y: 2, z: 1, core: 2. Of those that a mesh axis runs over, the one named last changes fastest.
Arguments:
- x_tok: bfloat16 [4096, 512], P('ty', 'tx')
- dy_tok: bfloat16 [4096, 512], P('ty', 'tx')
- ln_gain: float32 [512], P('tx')
- w_gate: bfloat16 [512, 2048], P('tx', 'ty')
- w_up: bfloat16 [512, 2048], P('tx', 'ty')
- w_down: bfloat16 [2048, 512], P('ty', 'tx')
Outputs:
- output 1: bfloat16 [4096, 512], P('ty', 'tx')
- output 2: bfloat16 [4096, 512], P('ty', 'tx')
- output 3: float32 [512, 2048], P('tx', 'ty')
- output 4: float32 [512, 2048], P('tx', 'ty')
- output 5: float32 [2048, 512], P('ty', 'tx')
- output 6: float32 [512], P('tx')
All inputs are finite; a program needn't handle non-finite values.
Results may differ from the reference program's by a relative error of at most 0.001.
Values are sent between devices in bfloat16 or wider.
A program may use at most 1 GiB of HBM per device.

```python
import jax
import jax.numpy as jnp
from jax import lax

TOKENS = 4096
D_MODEL = 512
D_FF = 2048
LN_EPS = 1e-6


def setup_inputs(seed: int = 0) -> dict:
    key_list = jax.random.split(jax.random.key(seed), 9)
    x_tok = (jax.random.normal(key_list[0], (TOKENS, D_MODEL), jnp.float32)
             + 1.5 * jax.random.normal(key_list[1], (TOKENS, 1), jnp.float32)).astype(jnp.bfloat16)
    dy_tok = jax.random.normal(key_list[2], (TOKENS, D_MODEL), jnp.float32).astype(jnp.bfloat16)
    ln_gain = 1.0 + 0.5 * jax.random.normal(key_list[3], (D_MODEL,), jnp.float32)
    in_scale = D_MODEL ** -0.5
    w_gate = ((jax.random.normal(key_list[4], (D_MODEL, D_FF), jnp.float32)
               + jax.random.normal(key_list[5], (1, D_FF), jnp.float32)) * in_scale).astype(jnp.bfloat16)
    w_up = ((jax.random.normal(key_list[6], (D_MODEL, D_FF), jnp.float32)
             + jax.random.normal(key_list[7], (1, D_FF), jnp.float32)) * in_scale).astype(jnp.bfloat16)
    w_down = (jax.random.normal(key_list[8], (D_FF, D_MODEL), jnp.float32) * D_FF ** -0.5).astype(jnp.bfloat16)
    return {"x_tok": x_tok, "dy_tok": dy_tok, "ln_gain": ln_gain,
            "w_gate": w_gate, "w_up": w_up, "w_down": w_down}


def reference(x_tok, dy_tok, ln_gain, w_gate, w_up, w_down):
    x_float = x_tok.astype(jnp.float32)
    mean_x = jnp.mean(x_float, axis=1, keepdims=True)
    mean_sq = jnp.mean(x_float * x_float, axis=1, keepdims=True)
    inv_std = lax.rsqrt(mean_sq - mean_x * mean_x + LN_EPS)
    x_hat = (x_float - mean_x) * inv_std
    h_norm = (ln_gain * x_hat).astype(jnp.bfloat16)
    gate_pre = jnp.dot(h_norm, w_gate, preferred_element_type=jnp.float32)
    up_pre = jnp.dot(h_norm, w_up, preferred_element_type=jnp.float32)
    gate_sig = jax.nn.sigmoid(gate_pre)
    gate_swish = gate_pre * gate_sig
    act_out = (gate_swish * up_pre).astype(jnp.bfloat16)
    mlp_out = jnp.dot(act_out, w_down, preferred_element_type=jnp.float32)
    y_tok = (x_float + mlp_out).astype(jnp.bfloat16)
    dw_down = jnp.dot(act_out.T, dy_tok, preferred_element_type=jnp.float32)
    d_act = jnp.dot(dy_tok, w_down.T, preferred_element_type=jnp.float32)
    d_gate = (d_act * up_pre * gate_sig * (1.0 + gate_pre * (1.0 - gate_sig))).astype(jnp.bfloat16)
    d_up = (d_act * gate_swish).astype(jnp.bfloat16)
    dw_gate = jnp.dot(h_norm.T, d_gate, preferred_element_type=jnp.float32)
    dw_up = jnp.dot(h_norm.T, d_up, preferred_element_type=jnp.float32)
    d_hnorm = (jnp.dot(d_gate, w_gate.T, preferred_element_type=jnp.float32)
               + jnp.dot(d_up, w_up.T, preferred_element_type=jnp.float32))
    d_gain = jnp.sum(d_hnorm * x_hat, axis=0)
    d_xhat = d_hnorm * ln_gain
    dx_ln = inv_std * (d_xhat - jnp.mean(d_xhat, axis=1, keepdims=True)
                       - x_hat * jnp.mean(d_xhat * x_hat, axis=1, keepdims=True))
    dx_tok = (dy_tok.astype(jnp.float32) + dx_ln).astype(jnp.bfloat16)
    return (y_tok, dx_tok, dw_gate, dw_up, dw_down, d_gain)
```

```python
import jax
import jax.numpy as jnp
from jax import lax
from jax.experimental import pallas as pl
from jax.experimental.pallas import tpu as pltpu
from jax.sharding import PartitionSpec as P

LN_EPS = 1e-6
MESH = pl.DeviceIdType.MESH
F32 = jnp.float32
BF16 = jnp.bfloat16

OWN, PAIR, NEAR, DIAG = 0, 1, 2, 3
CHUNKS = 4
LN_ROWS = 128
ROW_TILE = 256


def dot(a, b):
    return lax.dot_general(a, b, (((1,), (0,)), ((), ())), preferred_element_type=F32)


def dot_nt(a, b):
    return lax.dot_general(a, b, (((1,), (1,)), ((), ())), preferred_element_type=F32)


def kernel(x_in, dy_in, g_in, w1_in, w3_in, w2_in,
           y_out, dx_out, dw1_out, dw3_out, dw2_out, dg_out,
           xg, dyg, gg, w1g, w3g, w2g, h, h_t, dy_t, act, du, dv, part, pair_in, summed, link_in,
           m_acc, dh_acc, y_st, dx_st, dw_st, dw2_st, dg_st, dg_in,
           g_send, g_recv, in_send, in_recv, fw_send, fw_recv, w_send, w_recv, dw_send, dw_recv,
           lk_send, lk_recv, out_send, out_recv, dg_send, dg_recv, lc_in, lc_w, lc_g, lc_out, lc_dw):
    y, t = lax.axis_index("ty"), lax.axis_index("tx")
    x, c = t // 2, t % 2
    tok = x_in.shape[0] // 4
    wid = x_in.shape[1]
    fc = w1_in.shape[1] // CHUNKS
    d = 4 * wid
    peer_t = (t, 2 * x + 1 - c, 2 * (1 - x) + c, 2 * (1 - x) + 1 - c)
    dev = {r: (y, peer_t[r]) for r in (PAIR, NEAR, DIAG)}
    cross = (1 - y, t)

    barrier = pltpu.get_barrier_semaphore()
    for ya in (y, 1 - y):
        for r in range(4):
            if ya is y and r == OWN:
                continue
            pl.semaphore_signal(barrier, inc=1, device_id=(ya, peer_t[r]), device_id_type=MESH)
    pl.semaphore_wait(barrier, 7)

    def remote(src, dst, send, recv, to):
        return pltpu.make_async_remote_copy(src_ref=src, dst_ref=dst, send_sem=send, recv_sem=recv,
                                            device_id=to, device_id_type=MESH)

    def col(r):
        return pl.ds(pl.multiple_of(peer_t[r] * wid, wid), wid)

    def rows_of(r):
        return pl.ds(pl.multiple_of(peer_t[r] * tok, tok), tok)

    mine, other = pl.ds(0, tok), pl.ds(tok, tok)
    tin, tg = (x_in, dy_in), (xg, dyg)

    def in_copy(i, r):
        return remote(tin[i].at[rows_of(r), :], tg[i].at[mine, col(OWN)], in_send.at[i, r], in_recv.at[i, r], dev[r])

    def fw_copy(i, r):
        src = tin[i].at[rows_of(OWN), :] if r == OWN else tg[i].at[mine, col(r)]
        return remote(src, tg[i].at[other, col(r)], fw_send.at[i, r], fw_recv.at[i, r], cross)

    def own_copy(i):
        return pltpu.make_async_copy(tin[i].at[rows_of(OWN), :], tg[i].at[mine, col(OWN)], lc_in.at[i])

    def g_copy(r):
        return remote(g_in, gg.at[t], g_send.at[r], g_recv.at[r], dev[r])

    def w_src(w, j):
        if w == 2:
            return w2_in.at[pl.ds(j * fc, fc), :]
        return (w1_in, w3_in)[w].at[:, pl.ds(j * fc, fc)]

    def w_dst(w, j, r):
        if w == 2:
            return w2g.at[j, :, col(r)]
        return (w1g, w3g)[w].at[j, col(r), :]

    def w_copy(kind, w, j):
        if kind == 0:
            src, dst, to = w_src(w, j), w_dst(w, j, OWN), dev[NEAR]
        elif kind == 1:
            src, dst, to = w_src(w, j), w_dst(w, j, OWN), dev[PAIR]
        elif kind == 2:
            src, dst, to = w_dst(w, j, NEAR), w_dst(w, j, NEAR), dev[PAIR]
        elif kind == 3:
            src, dst, to = w_src(w, j), w_dst(w, CHUNKS + j, OWN), cross
        elif kind == 4:
            src, dst, to = w_dst(w, j, NEAR), w_dst(w, CHUNKS + j, NEAR), cross
        elif kind == 5:
            src, dst, to = w_dst(w, CHUNKS + j, OWN), w_dst(w, CHUNKS + j, OWN), dev[PAIR]
        else:
            src, dst, to = w_dst(w, CHUNKS + j, NEAR), w_dst(w, CHUNKS + j, NEAR), dev[PAIR]
        return remote(src, dst, w_send.at[kind, w, j], w_recv.at[kind, w, j], to)

    def own_w(w, j):
        return pltpu.make_async_copy(w_src(w, j), w_dst(w, j, OWN), lc_w.at[w, j])

    for r in (NEAR, DIAG):
        in_copy(0, r).start()
    for i in range(2):
        in_copy(i, PAIR).start()
        fw_copy(i, OWN).start()
    for r in (PAIR, NEAR, DIAG):
        g_copy(r).start()
    own_g = pltpu.make_async_copy(g_in, gg.at[t], lc_g)
    own_g.start()
    for i in range(2):
        own_copy(i).start()
    for r in (NEAR, DIAG):
        in_copy(1, r).start()
    for j in range(CHUNKS):
        for w in range(3):
            w_copy(0, w, j).start()
            w_copy(1, w, j).start()
            own_w(w, j).start()

    for i in range(2):
        in_copy(i, PAIR).wait_recv()
        fw_copy(i, PAIR).start()
    for r in (NEAR, DIAG):
        in_copy(0, r).wait_recv()
        fw_copy(0, r).start()
    own_copy(0).wait()
    own_g.wait()
    for r in (PAIR, NEAR, DIAG):
        g_copy(r).wait_recv()
    gain = jnp.concatenate([gg[k] for k in range(4)], axis=1)

    def norm(rows):
        xf = xg[rows, :].astype(F32)
        mu = jnp.sum(xf, axis=1, keepdims=True) * (1.0 / d)
        s = jnp.sum(xf * xf, axis=1, keepdims=True) * (1.0 / d)
        inv = lax.rsqrt(s - mu * mu + LN_EPS)
        return xf, (xf - mu) * inv, inv

    def ln_rows(base):
        def body(k, carry):
            rows = pl.ds(pl.multiple_of(base + k * LN_ROWS, LN_ROWS), LN_ROWS)
            _, xhat, _ = norm(rows)
            hb = (gain * xhat).astype(BF16)
            h[rows, :] = hb
            h_t[:, rows] = hb.astype(F32).T.astype(BF16)
            return carry
        lax.fori_loop(0, tok // LN_ROWS, body, 0)

    def dy_rows(base):
        def body(k, carry):
            rows = pl.ds(pl.multiple_of(base + k * LN_ROWS, LN_ROWS), LN_ROWS)
            dy_t[:, rows] = dyg[rows, :].astype(F32).T.astype(BF16)
            return carry
        lax.fori_loop(0, tok // LN_ROWS, body, 0)

    ln_rows(0)
    for r in (NEAR, DIAG):
        in_copy(1, r).wait_recv()
        fw_copy(1, r).start()
    own_copy(1).wait()
    dy_rows(0)

    def pass_w(j):
        for w in range(3):
            w_copy(3, w, j).start()
        for w in range(3):
            w_copy(0, w, j).wait_recv()
            w_copy(2, w, j).start()
            w_copy(4, w, j).start()

    pass_w(0)
    for r in range(4):
        fw_copy(0, r).wait_recv()
    ln_rows(tok)
    pass_w(1)
    for r in range(4):
        fw_copy(1, r).wait_recv()
    dy_rows(tok)

    m_acc[...] = jnp.zeros_like(m_acc)
    dh_acc[...] = jnp.zeros_like(dh_acc)

    def gated(j, n):
        def body(k, carry):
            rows = pl.ds(pl.multiple_of(k * ROW_TILE, ROW_TILE), ROW_TILE)
            hr = h[rows, :]
            u = dot(hr, w1g[j])
            v = dot(hr, w3g[j])
            da = dot_nt(dyg[rows, :], w2g[j])
            sig = 1.0 / (1.0 + jnp.exp(-u))
            swish = u * sig
            act[rows, :] = (swish * v).astype(BF16)
            du[rows, :] = (da * v * sig * (1.0 + u * (1.0 - sig))).astype(BF16)
            dv[rows, :] = (da * swish).astype(BF16)
            return carry
        lax.fori_loop(0, n // ROW_TILE, body, 0)

    def to_tokens(j):
        def body(k, carry):
            rows = pl.ds(pl.multiple_of(k * ROW_TILE, ROW_TILE), ROW_TILE)
            m_acc[rows, :] += dot(act[rows, :], w2g[j])
            dh_acc[rows, :] += dot_nt(du[rows, :], w1g[j]) + dot_nt(dv[rows, :], w3g[j])
            return carry
        lax.fori_loop(0, tok // ROW_TILE, body, 0)

    def pair_copy(far, j):
        block = peer_t[DIAG] if far else peer_t[PAIR]
        return remote(part.at[j, block], pair_in.at[far, j], dw_send.at[far, j], dw_recv.at[far, j], dev[PAIR])

    def link_copy(j):
        return remote(summed.at[j], link_in.at[j], lk_send.at[j], lk_recv.at[j], dev[NEAR])

    for j in range(CHUNKS):
        for w in range(3):
            own_w(w, j).wait()
            w_copy(1, w, j).wait_recv()
            w_copy(2, w, j).wait_recv()
        gated(j, 2 * tok)
        for k, (left, right) in enumerate(((h_t, du), (h_t, dv), (dy_t, act))):
            full = dot(left[...], right[...])
            for b in range(4):
                part[j, b, k * wid:(k + 1) * wid, :] = full[b * wid:(b + 1) * wid, :]
        pair_copy(1, j).start()
        pair_copy(0, j).start()
        to_tokens(j)
        pair_copy(1, j).wait_recv()
        summed[j] = part[j, peer_t[NEAR]] + pair_in[1, j]
        link_copy(j).start()
        if j + 2 < CHUNKS:
            pass_w(j + 2)

    def dw_outs(j):
        cols = pl.ds(j * fc, fc)
        return (pltpu.make_async_copy(dw_st.at[j, 0], dw1_out.at[:, cols], lc_dw.at[0, j]),
                pltpu.make_async_copy(dw_st.at[j, 1], dw3_out.at[:, cols], lc_dw.at[1, j]),
                pltpu.make_async_copy(dw2_st.at[j], dw2_out.at[cols, :], lc_dw.at[2, j]))

    def finish_dw(j):
        pair_copy(0, j).wait_recv()
        link_copy(j).wait_recv()
        total = part[j, t] + pair_in[0, j] + link_in[j]
        dw_st[j, 0] = total[:wid, :]
        dw_st[j, 1] = total[wid:2 * wid, :]
        dw2_st[j] = total[2 * wid:, :].T
        for cp in dw_outs(j):
            cp.start()

    for j in range(CHUNKS):
        for w in range(3):
            w_copy(3, w, j).wait_recv()
            w_copy(5, w, j).start()
        for w in range(3):
            w_copy(4, w, j).wait_recv()
            w_copy(6, w, j).start()
        for w in range(3):
            w_copy(5, w, j).wait_recv()
            w_copy(6, w, j).wait_recv()
        gated(CHUNKS + j, tok)
        to_tokens(CHUNKS + j)
        if j in (1, 2):
            finish_dw(j - 1)

    outs, stage = (y_out, dx_out), (y_st, dx_st)

    def out_copy(i, r):
        return remote(stage[i].at[:, col(r)], outs[i].at[rows_of(OWN), :], out_send.at[i, r], out_recv.at[i, r], dev[r])

    def own_out(i):
        return pltpu.make_async_copy(stage[i].at[:, col(OWN)], outs[i].at[rows_of(OWN), :], lc_out.at[i])

    def y_rows(k, carry):
        rows = pl.ds(pl.multiple_of(k * LN_ROWS, LN_ROWS), LN_ROWS)
        y_st[rows, :] = (xg[rows, :].astype(F32) + m_acc[rows, :]).astype(BF16)
        return carry

    def dx_rows(k, dg):
        rows = pl.ds(pl.multiple_of(k * LN_ROWS, LN_ROWS), LN_ROWS)
        _, xhat, inv = norm(rows)
        dh = dh_acc[rows, :]
        e = dh * gain
        me = jnp.sum(e, axis=1, keepdims=True) * (1.0 / d)
        mex = jnp.sum(e * xhat, axis=1, keepdims=True) * (1.0 / d)
        dx_st[rows, :] = (dyg[rows, :].astype(F32) + inv * (e - me - xhat * mex)).astype(BF16)
        return dg + jnp.sum(dh * xhat, axis=0, keepdims=True)

    lax.fori_loop(0, tok // LN_ROWS, y_rows, 0)
    for r in (NEAR, DIAG, PAIR):
        out_copy(0, r).start()
    own_out(0).start()
    dg = lax.fori_loop(0, tok // LN_ROWS, dx_rows, jnp.zeros((1, d), F32))
    for b in range(4):
        dg_st[b] = dg[:, b * wid:(b + 1) * wid]
    for r in (NEAR, DIAG, PAIR):
        out_copy(1, r).start()
    own_out(1).start()

    def dg_copy(a, r):
        ya = (y, 1 - y)[a]
        return remote(dg_st.at[peer_t[r]], dg_in.at[a, r], dg_send.at[a, r], dg_recv.at[a, r], (ya, peer_t[r]))

    dg_peers = [(a, r) for a in range(2) for r in range(4) if (a, r) != (0, OWN)]
    for a, r in dg_peers:
        dg_copy(a, r).start()

    finish_dw(CHUNKS - 2)
    finish_dw(CHUNKS - 1)

    total_dg = dg_st[t]
    for a, r in dg_peers:
        dg_copy(a, r).wait_recv()
        total_dg = total_dg + dg_in[a, r]
    dg_out[...] = total_dg

    for i in range(2):
        own_out(i).wait()
        for r in (PAIR, NEAR, DIAG):
            in_copy(i, r).wait_send()
            out_copy(i, r).wait_send()
            out_copy(i, r).wait_recv()
        for r in range(4):
            fw_copy(i, r).wait_send()
    for r in (PAIR, NEAR, DIAG):
        g_copy(r).wait_send()
    for a, r in dg_peers:
        dg_copy(a, r).wait_send()
    for j in range(CHUNKS):
        for kind in range(7):
            for w in range(3):
                w_copy(kind, w, j).wait_send()
        pair_copy(0, j).wait_send()
        pair_copy(1, j).wait_send()
        link_copy(j).wait_send()
        for cp in dw_outs(j):
            cp.wait()


def solution(mesh):
    def local_step(x_blk, dy_blk, gain_blk, w_gate_blk, w_up_blk, w_down_blk):
        rows, wid = x_blk.shape
        f = w_gate_blk.shape[1]
        tok, d, fc = rows // 4, 4 * wid, f // CHUNKS
        vm, dma = pltpu.VMEM, pltpu.SemaphoreType.DMA
        any_spec = pl.BlockSpec(memory_space=pl.ANY)
        outs = pl.pallas_call(
            kernel,
            name="mlp_branch",
            out_shape=(jax.ShapeDtypeStruct((rows, wid), BF16), jax.ShapeDtypeStruct((rows, wid), BF16),
                       jax.ShapeDtypeStruct((wid, f), F32), jax.ShapeDtypeStruct((wid, f), F32),
                       jax.ShapeDtypeStruct((f, wid), F32), jax.ShapeDtypeStruct((1, wid), F32)),
            in_specs=[any_spec] * 6,
            out_specs=(any_spec,) * 5 + (pl.BlockSpec(memory_space=pltpu.VMEM),),
            scratch_shapes=[
                vm((2 * tok, d), BF16), vm((2 * tok, d), BF16), vm((4, 1, wid), F32),
                vm((2 * CHUNKS, d, fc), BF16), vm((2 * CHUNKS, d, fc), BF16), vm((2 * CHUNKS, fc, d), BF16),
                vm((2 * tok, d), BF16), vm((d, 2 * tok), BF16), vm((d, 2 * tok), BF16),
                vm((2 * tok, fc), BF16), vm((2 * tok, fc), BF16), vm((2 * tok, fc), BF16),
                vm((CHUNKS, 4, 3 * wid, fc), F32), vm((2, CHUNKS, 3 * wid, fc), F32),
                vm((CHUNKS, 3 * wid, fc), F32), vm((CHUNKS, 3 * wid, fc), F32),
                vm((tok, d), F32), vm((tok, d), F32), vm((tok, d), BF16), vm((tok, d), BF16),
                vm((CHUNKS, 2, wid, fc), F32), vm((CHUNKS, fc, wid), F32),
                vm((4, 1, wid), F32), vm((2, 4, 1, wid), F32),
                dma((4,)), dma((4,)), dma((2, 4)), dma((2, 4)), dma((2, 4)), dma((2, 4)),
                dma((7, 3, CHUNKS)), dma((7, 3, CHUNKS)), dma((2, CHUNKS)), dma((2, CHUNKS)),
                dma((CHUNKS,)), dma((CHUNKS,)), dma((2, 4)), dma((2, 4)), dma((2, 4)), dma((2, 4)),
                dma((2,)), dma((3, CHUNKS)), dma(()), dma((2,)), dma((3, CHUNKS)),
            ],
            compiler_params=pltpu.CompilerParams(collective_id=0, has_side_effects=True,
                                                 vmem_limit_bytes=60 * 2 ** 20),
        )(x_blk, dy_blk, gain_blk.reshape(1, wid), w_gate_blk, w_up_blk, w_down_blk)
        return outs[:5] + (outs[5].reshape(wid),)

    return jax.shard_map(
        local_step, mesh=mesh,
        in_specs=(P("ty", "tx"), P("ty", "tx"), P("tx"), P("tx", "ty"), P("tx", "ty"), P("ty", "tx")),
        out_specs=(P("ty", "tx"), P("ty", "tx"), P("tx", "ty"), P("tx", "ty"), P("ty", "tx"), P("tx")),
        check_vma=False)
```

```python
import jax
import jax.numpy as jnp
from jax import lax
from jax.experimental import pallas as pl
from jax.experimental.pallas import tpu as pltpu
from jax.sharding import PartitionSpec as P

LN_EPS = 1e-6
MESH = pl.DeviceIdType.MESH
F32 = jnp.float32
BF16 = jnp.bfloat16

OWN, PAIR, NEAR, DIAG = 0, 1, 2, 3
CHUNKS = 4
LN_ROWS = 128
ROW_TILE = 256


def dot(a, b):
    return lax.dot_general(a, b, (((1,), (0,)), ((), ())), preferred_element_type=F32)


def dot_nt(a, b):
    return lax.dot_general(a, b, (((1,), (1,)), ((), ())), preferred_element_type=F32)


def kernel(x_in, dy_in, g_in, w1_in, w3_in, w2_in,
           y_out, dx_out, dw1_out, dw3_out, dw2_out, dg_out,
           xg, dyg, gg, w1g, w3g, w2g, h, h_t, dy_t, act, du, dv, part, pair_in, summed, link_in,
           m_acc, dh_acc, y_st, dx_st, dw_st, dw2_st, dg_st, dg_in, st_own, st_in,
           g_send, g_recv, in_send, in_recv, w_send, w_recv, dw_send, dw_recv,
           lk_send, lk_recv, out_send, out_recv, dg_send, dg_recv, st_send, st_recv, lc_in, lc_w, lc_g, lc_out, lc_dw):
    y, t = lax.axis_index("ty"), lax.axis_index("tx")
    x, c = t // 2, t % 2
    tok = x_in.shape[0] // 2
    wid = x_in.shape[1]
    fc = w1_in.shape[1] // CHUNKS
    d = 4 * wid
    half = 2 * wid
    peer_t = (t, 2 * x + 1 - c, 2 * (1 - x) + c, 2 * (1 - x) + 1 - c)
    peer_c = (c, 1 - c, c, 1 - c)
    dev = {r: (y, peer_t[r]) for r in (PAIR, NEAR, DIAG)}
    cross, cross_pair = (1 - y, t), (1 - y, peer_t[PAIR])

    barrier = pltpu.get_barrier_semaphore()
    for to in (dev[PAIR], dev[NEAR], dev[DIAG], cross, cross_pair):
        pl.semaphore_signal(barrier, inc=1, device_id=to, device_id_type=MESH)
    pl.semaphore_wait(barrier, 5)

    def remote(src, dst, send, recv, to):
        return pltpu.make_async_remote_copy(src_ref=src, dst_ref=dst, send_sem=send, recv_sem=recv,
                                            device_id=to, device_id_type=MESH)

    def col(r):
        return pl.ds(pl.multiple_of(peer_t[r] * wid, wid), wid)

    def rows_of(core):
        return pl.ds(pl.multiple_of(core * tok, tok), tok)

    chip = pl.ds(pl.multiple_of(x * half, half), half)
    tin, tg = (x_in, dy_in), (xg, dyg)

    def in_copy(i, r):
        return remote(tin[i].at[rows_of(peer_c[r]), :], tg[i].at[:, col(OWN)], in_send.at[i, r], in_recv.at[i, r], dev[r])

    def own_copy(i):
        return pltpu.make_async_copy(tin[i].at[rows_of(c), :], tg[i].at[:, col(OWN)], lc_in.at[i])

    def g_copy(r):
        return remote(g_in, gg.at[t], g_send.at[r], g_recv.at[r], dev[r])

    def w_src(w, j):
        if w == 2:
            return w2_in.at[pl.ds(j * fc, fc), :]
        return (w1_in, w3_in)[w].at[:, pl.ds(j * fc, fc)]

    def w_dst(w, j, r):
        if w == 2:
            return w2g.at[j, :, col(r)]
        return (w1g, w3g)[w].at[j, col(r), :]

    def w_copy(kind, w, j):
        if kind == 0:
            src, dst, to = w_src(w, j), w_dst(w, j, OWN), dev[NEAR]
        elif kind == 1:
            src, dst, to = w_src(w, j), w_dst(w, j, OWN), dev[PAIR]
        elif kind == 2:
            src, dst, to = w_dst(w, j, NEAR), w_dst(w, j, NEAR), dev[PAIR]
        elif kind == 3:
            src, dst, to = w_src(w, j), w_dst(w, CHUNKS + j, OWN), cross
        elif kind == 4:
            src, dst, to = w_dst(w, CHUNKS + j, OWN), w_dst(w, CHUNKS + j, OWN), dev[NEAR]
        elif kind == 5:
            src, dst, to = w_dst(w, CHUNKS + j, OWN), w_dst(w, CHUNKS + j, OWN), dev[PAIR]
        else:
            src, dst, to = w_dst(w, CHUNKS + j, NEAR), w_dst(w, CHUNKS + j, NEAR), dev[PAIR]
        return remote(src, dst, w_send.at[kind, w, j], w_recv.at[kind, w, j], to)

    def own_w(w, j):
        return pltpu.make_async_copy(w_src(w, j), w_dst(w, j, OWN), lc_w.at[w, j])

    for i in range(2):
        for r in (NEAR, DIAG):
            in_copy(i, r).start()
    for j in range(CHUNKS):
        for w in range(3):
            w_copy(3, w, j).start()
    for i in range(2):
        in_copy(i, PAIR).start()
        own_copy(i).start()
    for r in (PAIR, NEAR, DIAG):
        g_copy(r).start()
    own_g = pltpu.make_async_copy(g_in, gg.at[t], lc_g)
    own_g.start()
    for j in range(CHUNKS):
        for w in range(3):
            w_copy(1, w, j).start()
            own_w(w, j).start()

    def pass_cross(j):
        for w in range(3):
            w_copy(3, w, j).wait_recv()
            w_copy(4, w, j).start()
            w_copy(5, w, j).start()

    pass_cross(0)
    pass_cross(1)
    own_copy(0).wait()
    own_g.wait()
    for r in (PAIR, NEAR, DIAG):
        in_copy(0, r).wait_recv()
        g_copy(r).wait_recv()
    gain = jnp.concatenate([gg[k] for k in range(4)], axis=1)
    gain_chip = jnp.concatenate([gg[2 * x], gg[2 * x + 1]], axis=1)

    def stats(rows):
        xf = xg[rows, :].astype(F32)
        mu = jnp.sum(xf, axis=1, keepdims=True) * (1.0 / d)
        s = jnp.sum(xf * xf, axis=1, keepdims=True) * (1.0 / d)
        return xf, mu, lax.rsqrt(s - mu * mu + LN_EPS)

    def blocks(n, body, carry=0):
        def step(k, carry):
            return body(k, pl.ds(pl.multiple_of(k * n, n), n), carry)
        return lax.fori_loop(0, tok // n, step, carry)

    def ln_rows(k, rows, carry):
        xf, mu, inv = stats(rows)
        h[rows, :] = (gain * ((xf - mu) * inv)).astype(BF16)
        h_t[:, rows] = h[rows, chip].astype(F32).T.astype(BF16)
        return carry

    def dy_rows(k, rows, carry):
        dy_t[:, rows] = dyg[rows, chip].astype(F32).T.astype(BF16)
        return carry

    blocks(LN_ROWS, ln_rows)
    m_acc[...] = jnp.zeros_like(m_acc)
    dh_acc[...] = jnp.zeros_like(dh_acc)
    for j in range(2, CHUNKS):
        pass_cross(j)
    for j in range(CHUNKS):
        for w in range(3):
            w_copy(0, w, j).start()
    own_copy(1).wait()
    for r in (PAIR, NEAR, DIAG):
        in_copy(1, r).wait_recv()
    blocks(LN_ROWS, dy_rows)

    def gated(j):
        def body(k, rows, carry):
            hr = h[rows, :]
            u = dot(hr, w1g[j])
            v = dot(hr, w3g[j])
            da = dot_nt(dyg[rows, :], w2g[j])
            sig = 1.0 / (1.0 + jnp.exp(-u))
            swish = u * sig
            act[rows, :] = (swish * v).astype(BF16)
            du[rows, :] = (da * v * sig * (1.0 + u * (1.0 - sig))).astype(BF16)
            dv[rows, :] = (da * swish).astype(BF16)
            return carry
        blocks(ROW_TILE, body)

    def weight_grads(j):
        for k, (left, right) in enumerate(((h_t, du), (h_t, dv), (dy_t, act))):
            full = dot(left[...], right[...])
            for b in range(2):
                part[j, b, k * wid:(k + 1) * wid, :] = full[b * wid:(b + 1) * wid, :]

    def to_tokens(j):
        def body(k, rows, carry):
            m_acc[rows, :] += dot(act[rows, :], w2g[j, :, chip])
            dh_acc[rows, :] += dot_nt(du[rows, :], w1g[j, chip, :]) + dot_nt(dv[rows, :], w3g[j, chip, :])
            return carry
        blocks(ROW_TILE, body)

    def pair_copy(j):
        return remote(part.at[j, 1 - c], pair_in.at[j], dw_send.at[j], dw_recv.at[j], dev[PAIR])

    def link_copy(j):
        return remote(summed.at[j], link_in.at[j], lk_send.at[j], lk_recv.at[j], cross)

    for j in range(CHUNKS):
        for w in range(3):
            w_copy(4, w, j).wait_recv()
            w_copy(6, w, j).start()
        for w in range(3):
            w_copy(5, w, j).wait_recv()
            w_copy(6, w, j).wait_recv()
        gated(CHUNKS + j)
        weight_grads(CHUNKS + j)
        pair_copy(CHUNKS + j).start()
        to_tokens(CHUNKS + j)
        pair_copy(CHUNKS + j).wait_recv()
        summed[j] = part[CHUNKS + j, c] + pair_in[CHUNKS + j]
        link_copy(j).start()

    for j in range(CHUNKS):
        for w in range(3):
            w_copy(0, w, j).wait_recv()
            w_copy(2, w, j).start()
        for w in range(3):
            own_w(w, j).wait()
            w_copy(1, w, j).wait_recv()
            w_copy(2, w, j).wait_recv()
        gated(j)
        weight_grads(j)
        pair_copy(j).start()
        to_tokens(j)

    outs, stage = (y_out, dx_out), (y_st, dx_st)

    def part_cols(core):
        return pl.ds(pl.multiple_of(core * wid, wid), wid)

    def out_copy(i):
        return remote(stage[i].at[:, part_cols(1 - c)], outs[i].at[rows_of(c), :], out_send.at[i], out_recv.at[i], dev[PAIR])

    def own_out(i):
        return pltpu.make_async_copy(stage[i].at[:, part_cols(c)], outs[i].at[rows_of(c), :], lc_out.at[i])

    lane = lax.broadcasted_iota(jnp.int32, (LN_ROWS, LN_ROWS), 1)

    def sum_rows(k, rows, dg):
        _, mu, inv = stats(rows)
        xhat = (xg[rows, chip].astype(F32) - mu) * inv
        dh = dh_acc[rows, :]
        e = dh * gain_chip
        se = jnp.sum(e, axis=1, keepdims=True)
        sex = jnp.sum(e * xhat, axis=1, keepdims=True)
        st_own[k] = jnp.where(lane == 0, se, jnp.where(lane == 1, sex, 0.0)).T[:8, :]
        return dg + jnp.sum(dh * xhat, axis=0, keepdims=True)

    dg = blocks(LN_ROWS, sum_rows, jnp.zeros((1, half), F32))
    st_copy = remote(st_own, st_in, st_send, st_recv, dev[NEAR])
    st_copy.start()

    def y_rows(k, rows, carry):
        y_st[rows, :] = (xg[rows, chip].astype(F32) + m_acc[rows, :]).astype(BF16)
        return carry

    blocks(LN_ROWS, y_rows)
    out_copy(0).start()
    own_out(0).start()
    for b in range(2):
        dg_st[b] = dg[:, b * wid:(b + 1) * wid]
    dg_copies = [remote(dg_st.at[b], dg_in.at[k], dg_send.at[k], dg_recv.at[k], to)
                 for k, (b, to) in enumerate(((1 - c, dev[PAIR]), (c, cross), (1 - c, cross_pair)))]
    for cp in dg_copies:
        cp.start()

    st_copy.wait_recv()

    def dx_rows(k, rows, carry):
        _, mu, inv = stats(rows)
        xhat = (xg[rows, chip].astype(F32) - mu) * inv
        e = dh_acc[rows, :] * gain_chip
        both = jnp.concatenate([st_own[k] + st_in[k], jnp.zeros((LN_ROWS - 8, LN_ROWS), F32)], axis=0).T * (1.0 / d)
        dx = dyg[rows, chip].astype(F32) + inv * (e - both[:, 0:1] - xhat * both[:, 1:2])
        dx_st[rows, :] = dx.astype(BF16)
        return carry

    blocks(LN_ROWS, dx_rows)
    out_copy(1).start()
    own_out(1).start()

    def dw_outs(j):
        cols = pl.ds(j * fc, fc)
        return (pltpu.make_async_copy(dw_st.at[j, 0], dw1_out.at[:, cols], lc_dw.at[0, j]),
                pltpu.make_async_copy(dw_st.at[j, 1], dw3_out.at[:, cols], lc_dw.at[1, j]),
                pltpu.make_async_copy(dw2_st.at[j], dw2_out.at[cols, :], lc_dw.at[2, j]))

    for j in range(CHUNKS):
        pair_copy(j).wait_recv()
        link_copy(j).wait_recv()
        total = part[j, c] + pair_in[j] + link_in[j]
        dw_st[j, 0] = total[:wid, :]
        dw_st[j, 1] = total[wid:2 * wid, :]
        dw2_st[j] = total[2 * wid:, :].T
        for cp in dw_outs(j):
            cp.start()

    total_dg = dg_st[c]
    for k, cp in enumerate(dg_copies):
        cp.wait_recv()
        total_dg = total_dg + dg_in[k]
    dg_out[...] = total_dg

    for i in range(2):
        own_out(i).wait()
        out_copy(i).wait_send()
        out_copy(i).wait_recv()
        for r in (PAIR, NEAR, DIAG):
            in_copy(i, r).wait_send()
    for r in (PAIR, NEAR, DIAG):
        g_copy(r).wait_send()
    for cp in dg_copies:
        cp.wait_send()
    st_copy.wait_send()
    for j in range(CHUNKS):
        for kind in range(7):
            for w in range(3):
                w_copy(kind, w, j).wait_send()
        pair_copy(j).wait_send()
        pair_copy(CHUNKS + j).wait_send()
        link_copy(j).wait_send()
        for cp in dw_outs(j):
            cp.wait()


def solution(mesh):
    def local_step(x_blk, dy_blk, gain_blk, w_gate_blk, w_up_blk, w_down_blk):
        rows, wid = x_blk.shape
        f = w_gate_blk.shape[1]
        tok, d, half, fc = rows // 2, 4 * wid, 2 * wid, f // CHUNKS
        vm, dma = pltpu.VMEM, pltpu.SemaphoreType.DMA
        any_spec = pl.BlockSpec(memory_space=pl.ANY)
        outs = pl.pallas_call(
            kernel,
            name="mlp_branch",
            out_shape=(jax.ShapeDtypeStruct((rows, wid), BF16), jax.ShapeDtypeStruct((rows, wid), BF16),
                       jax.ShapeDtypeStruct((wid, f), F32), jax.ShapeDtypeStruct((wid, f), F32),
                       jax.ShapeDtypeStruct((f, wid), F32), jax.ShapeDtypeStruct((1, wid), F32)),
            in_specs=[any_spec] * 6,
            out_specs=(any_spec,) * 5 + (pl.BlockSpec(memory_space=pltpu.VMEM),),
            scratch_shapes=[
                vm((tok, d), BF16), vm((tok, d), BF16), vm((4, 1, wid), F32),
                vm((2 * CHUNKS, d, fc), BF16), vm((2 * CHUNKS, d, fc), BF16), vm((2 * CHUNKS, fc, d), BF16),
                vm((tok, d), BF16), vm((half, tok), BF16), vm((half, tok), BF16),
                vm((tok, fc), BF16), vm((tok, fc), BF16), vm((tok, fc), BF16),
                vm((2 * CHUNKS, 2, 3 * wid, fc), F32), vm((2 * CHUNKS, 3 * wid, fc), F32),
                vm((CHUNKS, 3 * wid, fc), F32), vm((CHUNKS, 3 * wid, fc), F32),
                vm((tok, half), F32), vm((tok, half), F32), vm((tok, half), BF16), vm((tok, half), BF16),
                vm((CHUNKS, 2, wid, fc), F32), vm((CHUNKS, fc, wid), F32),
                vm((2, 1, wid), F32), vm((3, 1, wid), F32),
                vm((tok // LN_ROWS, 8, LN_ROWS), F32), vm((tok // LN_ROWS, 8, LN_ROWS), F32),
                dma((4,)), dma((4,)), dma((2, 4)), dma((2, 4)),
                dma((7, 3, CHUNKS)), dma((7, 3, CHUNKS)), dma((2 * CHUNKS,)), dma((2 * CHUNKS,)),
                dma((CHUNKS,)), dma((CHUNKS,)), dma((2,)), dma((2,)), dma((3,)), dma((3,)), dma(()), dma(()),
                dma((2,)), dma((3, CHUNKS)), dma(()), dma((2,)), dma((3, CHUNKS)),
            ],
            compiler_params=pltpu.CompilerParams(collective_id=0, has_side_effects=True,
                                                 vmem_limit_bytes=60 * 2 ** 20),
        )(x_blk, dy_blk, gain_blk.reshape(1, wid), w_gate_blk, w_up_blk, w_down_blk)
        return outs[:5] + (outs[5].reshape(wid),)

    return jax.shard_map(
        local_step, mesh=mesh,
        in_specs=(P("ty", "tx"), P("ty", "tx"), P("tx"), P("tx", "ty"), P("tx", "ty"), P("ty", "tx")),
        out_specs=(P("ty", "tx"), P("ty", "tx"), P("tx", "ty"), P("tx", "ty"), P("ty", "tx"), P("tx")),
        check_vma=False)
```

```python
import jax
import jax.numpy as jnp
from jax import lax
from jax.experimental import pallas as pl
from jax.experimental.pallas import tpu as pltpu
from jax.sharding import PartitionSpec as P

LN_EPS = 1e-6
MESH = pl.DeviceIdType.MESH
F32 = jnp.float32
BF16 = jnp.bfloat16

OWN, PAIR, NEAR, DIAG = 0, 1, 2, 3
EIGHTHS = (1, 2, 2, 2, 1)
CHUNKS = len(EIGHTHS)
LN_ROWS = 128
ROW_TILE = 256


def dot(a, b):
    return lax.dot_general(a, b, (((1,), (0,)), ((), ())), preferred_element_type=F32)


def dot_nt(a, b):
    return lax.dot_general(a, b, (((1,), (1,)), ((), ())), preferred_element_type=F32)


def kernel(x_in, dy_in, g_in, w1_in, w3_in, w2_in,
           y_out, dx_out, dw1_out, dw3_out, dw2_out, dg_out,
           xg, dyg, gg, w1g, w3g, w2g, h, h_t, dy_t, xhat, inv_std, act, du, dv, part, pair_in, summed, link_in,
           m_acc, dh_acc, y_st, dx_st, dg_st, dg_in, st_own, st_in,
           g_send, g_recv, in_send, in_recv, w_send, w_recv, dw_send, dw_recv,
           lk_send, lk_recv, out_send, out_recv, dg_send, dg_recv, st_send, st_recv, lc_in, lc_w, lc_g):
    y, t = lax.axis_index("ty"), lax.axis_index("tx")
    x, c = t // 2, t % 2
    tok = x_in.shape[0] // 2
    wid = x_in.shape[1]
    d = 4 * wid
    half = 2 * wid
    unit = w1_in.shape[1] // 8
    size = [e * unit for e in EIGHTHS]
    start = [sum(size[:i]) for i in range(CHUNKS)]
    span = [pl.ds(start[i], size[i]) for i in range(CHUNKS)]
    peer_t = (t, 2 * x + 1 - c, 2 * (1 - x) + c, 2 * (1 - x) + 1 - c)
    peer_c = (c, 1 - c, c, 1 - c)
    dev = {r: (y, peer_t[r]) for r in (PAIR, NEAR, DIAG)}
    cross, cross_pair = (1 - y, t), (1 - y, peer_t[PAIR])

    barrier = pltpu.get_barrier_semaphore()
    for to in (dev[PAIR], dev[NEAR], dev[DIAG], cross, cross_pair):
        pl.semaphore_signal(barrier, inc=1, device_id=to, device_id_type=MESH)
    pl.semaphore_wait(barrier, 5)

    def remote(src, dst, send, recv, to):
        return pltpu.make_async_remote_copy(src_ref=src, dst_ref=dst, send_sem=send, recv_sem=recv,
                                            device_id=to, device_id_type=MESH)

    def col(r):
        return pl.ds(pl.multiple_of(peer_t[r] * wid, wid), wid)

    def rows_of(core):
        return pl.ds(pl.multiple_of(core * tok, tok), tok)

    def core_cols(core):
        return pl.ds(pl.multiple_of(core * wid, wid), wid)

    chip = pl.ds(pl.multiple_of(x * half, half), half)
    tin, tg = (x_in, dy_in), (xg, dyg)

    def in_copy(i, r):
        return remote(tin[i].at[rows_of(peer_c[r]), :], tg[i].at[:, col(OWN)], in_send.at[i, r], in_recv.at[i, r], dev[r])

    def own_copy(i):
        return pltpu.make_async_copy(tin[i].at[rows_of(c), :], tg[i].at[:, col(OWN)], lc_in.at[i])

    def g_copy(r):
        return remote(g_in, gg.at[t], g_send.at[r], g_recv.at[r], dev[r])

    def w_src(w, j):
        if w == 2:
            return w2_in.at[span[j], :]
        return (w1_in, w3_in)[w].at[:, span[j]]

    def w_dst(w, side, j, r):
        if w == 2:
            return w2g.at[side, span[j], col(r)]
        return (w1g, w3g)[w].at[side, col(r), span[j]]

    def w_copy(kind, w, j):
        if kind == 0:
            src, dst, to = w_src(w, j), w_dst(w, 0, j, OWN), dev[NEAR]
        elif kind == 1:
            src, dst, to = w_src(w, j), w_dst(w, 0, j, OWN), dev[PAIR]
        elif kind == 2:
            src, dst, to = w_dst(w, 0, j, NEAR), w_dst(w, 0, j, NEAR), dev[PAIR]
        elif kind == 3:
            src, dst, to = w_src(w, j), w_dst(w, 1, j, OWN), cross
        elif kind == 4:
            src, dst, to = w_dst(w, 1, j, OWN), w_dst(w, 1, j, OWN), dev[NEAR]
        elif kind == 5:
            src, dst, to = w_dst(w, 1, j, OWN), w_dst(w, 1, j, OWN), dev[PAIR]
        else:
            src, dst, to = w_dst(w, 1, j, NEAR), w_dst(w, 1, j, NEAR), dev[PAIR]
        return remote(src, dst, w_send.at[kind, w, j], w_recv.at[kind, w, j], to)

    def own_w(w, j):
        return pltpu.make_async_copy(w_src(w, j), w_dst(w, 0, j, OWN), lc_w.at[w, j])

    for i in range(2):
        for r in (NEAR, DIAG):
            in_copy(i, r).start()
    for j in range(CHUNKS):
        for w in range(3):
            w_copy(3, w, j).start()
    for i in range(2):
        in_copy(i, PAIR).start()
        own_copy(i).start()
    for r in (PAIR, NEAR, DIAG):
        g_copy(r).start()
    own_g = pltpu.make_async_copy(g_in, gg.at[t], lc_g)
    own_g.start()
    for j in range(CHUNKS):
        for w in range(3):
            w_copy(1, w, j).start()
            own_w(w, j).start()

    def pass_cross(j):
        for w in range(3):
            w_copy(3, w, j).wait_recv()
            w_copy(4, w, j).start()
            w_copy(5, w, j).start()

    pass_cross(0)
    pass_cross(1)
    own_copy(0).wait()
    own_g.wait()
    for r in (PAIR, NEAR, DIAG):
        in_copy(0, r).wait_recv()
        g_copy(r).wait_recv()
    gain = jnp.concatenate([gg[k] for k in range(4)], axis=1)
    gain_chip = jnp.concatenate([gg[2 * x], gg[2 * x + 1]], axis=1)

    def blocks(n, body, carry=0, lo=0, hi=None):
        def step(k, carry):
            return body(k, pl.ds(pl.multiple_of(k * n, n), n), carry)
        return lax.fori_loop(lo // n, (tok if hi is None else hi) // n, step, carry)

    def ln_rows(k, rows, carry):
        xf = xg[rows, :].astype(F32)
        mu = jnp.sum(xf, axis=1, keepdims=True) * (1.0 / d)
        s = jnp.sum(xf * xf, axis=1, keepdims=True) * (1.0 / d)
        inv = lax.rsqrt(s - mu * mu + LN_EPS)
        xh = (xf - mu) * inv
        xhat[rows, :] = xh
        inv_std[rows, :] = inv
        h[rows, :] = (gain * xh).astype(BF16)
        h_t[:, rows] = h[rows, chip].astype(F32).T.astype(BF16)
        return carry

    def dy_rows(k, rows, carry):
        dy_t[:, rows] = dyg[rows, chip].astype(F32).T.astype(BF16)
        return carry

    blocks(LN_ROWS, ln_rows)
    for j in range(2, CHUNKS):
        pass_cross(j)
    for j in range(CHUNKS):
        for w in range(3):
            w_copy(0, w, j).start()
    own_copy(1).wait()
    for r in (PAIR, NEAR, DIAG):
        in_copy(1, r).wait_recv()
    blocks(LN_ROWS, dy_rows)

    def gated(s, j):
        n = size[j]

        def body(k, rows, carry):
            hr = h[rows, :]
            u = dot(hr, w1g[s, :, span[j]])
            v = dot(hr, w3g[s, :, span[j]])
            da = dot_nt(dyg[rows, :], w2g[s, span[j], :])
            sig = 1.0 / (1.0 + jnp.exp(-u))
            swish = u * sig
            act[rows, :n] = (swish * v).astype(BF16)
            du[rows, :n] = (da * v * sig * (1.0 + u * (1.0 - sig))).astype(BF16)
            dv[rows, :n] = (da * swish).astype(BF16)
            return carry
        blocks(ROW_TILE, body)

    def pair_copy(s, j, k):
        band = pl.ds(k * wid, wid)
        return remote(part.at[s, 1 - c, band, span[j]], pair_in.at[s, band, span[j]],
                      dw_send.at[s, j, k], dw_recv.at[s, j, k], dev[PAIR])

    def weight_grads(s, j):
        for k, (left, right) in enumerate(((h_t, du), (h_t, dv), (dy_t, act))):
            full = dot(left[...], right[:, :size[j]])
            for b in range(2):
                part[s, b, k * wid:(k + 1) * wid, span[j]] = full[b * wid:(b + 1) * wid, :]
            pair_copy(s, j, k).start()

    def link_copy(j, k):
        band = pl.ds(k * wid, wid)
        return remote(summed.at[band, span[j]], link_in.at[band, span[j]], lk_send.at[j, k], lk_recv.at[j, k], cross)

    def send_sums(j):
        for k in range(3):
            band = pl.ds(k * wid, wid)
            pair_copy(1, j, k).wait_recv()
            summed[band, span[j]] = part[1, c, band, span[j]] + pair_in[1, band, span[j]]
            link_copy(j, k).start()

    def token_sums(s, j, rows):
        n = size[j]
        m = dot(act[rows, :n], w2g[s, span[j], chip])
        dh = dot_nt(du[rows, :n], w1g[s, chip, span[j]]) + dot_nt(dv[rows, :n], w3g[s, chip, span[j]])
        return m, dh

    def to_tokens(s, j, first=False):
        def body(k, rows, carry):
            m, dh = token_sums(s, j, rows)
            if first:
                m_acc[rows, :] = m
                dh_acc[rows, :] = dh
            else:
                m_acc[rows, :] += m
                dh_acc[rows, :] += dh
            return carry
        blocks(ROW_TILE, body)

    def pass_near(kind, j):
        for w in range(3):
            w_copy(kind, w, j).wait_recv()
            w_copy(6 if kind == 4 else 2, w, j).start()

    pass_near(4, 0)
    for j in range(CHUNKS):
        for w in range(3):
            w_copy(5, w, j).wait_recv()
            w_copy(6, w, j).wait_recv()
        gated(1, j)
        weight_grads(1, j)
        if j == 0:
            send_sums(j)
        to_tokens(1, j, first=j == 0)
        if j + 1 < CHUNKS:
            pass_near(4, j + 1)
        else:
            pass_near(0, 0)
        if j:
            send_sums(j)

    def finish_dw(j):
        for k in range(3):
            pair_copy(0, j, k).wait_recv()
            link_copy(j, k).wait_recv()
            band = pl.ds(k * wid, wid)
            total = part[0, c, band, span[j]] + pair_in[0, band, span[j]] + link_in[band, span[j]]
            if k == 2:
                dw2_out[span[j], :] = total.T
            else:
                (dw1_out, dw3_out)[k][:, span[j]] = total

    lane = lax.broadcasted_iota(jnp.int32, (LN_ROWS, LN_ROWS), 1)
    last = CHUNKS - 1

    def last_rows(k, rows, dg):
        m, dh = token_sums(0, last, rows)
        m_acc[rows, :] += m
        dh = dh_acc[rows, :] + dh
        dh_acc[rows, :] = dh
        xh = xhat[rows, chip]
        e = dh * gain_chip
        se = jnp.sum(e, axis=1, keepdims=True)
        sex = jnp.sum(e * xh, axis=1, keepdims=True)
        st_own[k] = jnp.where(lane == 0, se, jnp.where(lane == 1, sex, 0.0)).T[:8, :]
        return dg + jnp.sum(dh * xh, axis=0, keepdims=True)

    for j in range(CHUNKS):
        for w in range(3):
            own_w(w, j).wait()
            w_copy(1, w, j).wait_recv()
            w_copy(2, w, j).wait_recv()
        gated(0, j)
        if j < last:
            weight_grads(0, j)
            to_tokens(0, j)
            pass_near(0, j + 1)
            if j:
                finish_dw(j - 1)

    dg = blocks(LN_ROWS, last_rows, jnp.zeros((1, half), F32))
    st_copy = remote(st_own, st_in, st_send, st_recv, dev[NEAR])
    st_copy.start()
    weight_grads(0, last)

    outs, stage = (y_out, dx_out), (y_st, dx_st)
    mid = tok // 2

    def out_copy(i, part_of):
        rows = pl.ds(part_of * mid, mid)
        to_rows = pl.ds(pl.multiple_of(c * tok + part_of * mid, mid), mid)
        src = y_st.at[rows, :] if i == 0 else dx_st.at[rows, core_cols(1 - c)]
        return remote(src, outs[i].at[to_rows, :], out_send.at[i, part_of], out_recv.at[i, part_of], dev[PAIR])

    def out_rows(k):
        return pl.ds(pl.multiple_of(c * tok + k * LN_ROWS, LN_ROWS), LN_ROWS)

    def y_rows(k, rows, carry):
        y_st[rows, :] = (xg[rows, col(PAIR)].astype(F32) + m_acc[rows, core_cols(1 - c)]).astype(BF16)
        y_out[out_rows(k), :] = (xg[rows, col(OWN)].astype(F32) + m_acc[rows, core_cols(c)]).astype(BF16)
        return carry

    blocks(LN_ROWS, y_rows)
    for b in range(2):
        dg_st[b] = dg[:, b * wid:(b + 1) * wid]
        out_copy(0, b).start()
    dg_copies = [remote(dg_st.at[b], dg_in.at[k], dg_send.at[k], dg_recv.at[k], to)
                 for k, (b, to) in enumerate(((1 - c, dev[PAIR]), (c, cross), (1 - c, cross_pair)))]
    for cp in dg_copies:
        cp.start()

    st_copy.wait_recv()

    def dx_rows(k, rows, carry):
        both = jnp.concatenate([st_own[k] + st_in[k], jnp.zeros((LN_ROWS - 8, LN_ROWS), F32)], axis=0).T * (1.0 / d)
        e = dh_acc[rows, :] * gain_chip
        dx_ln = inv_std[rows, :] * (e - both[:, 0:1] - xhat[rows, chip] * both[:, 1:2])
        dx_st[rows, :] = (dyg[rows, chip].astype(F32) + dx_ln).astype(BF16)
        dx_out[out_rows(k), :] = dx_st[rows, core_cols(c)]
        return carry

    for b in range(2):
        blocks(LN_ROWS, dx_rows, lo=b * mid, hi=(b + 1) * mid)
        out_copy(1, b).start()

    finish_dw(last - 1)
    finish_dw(last)

    total_dg = dg_st[c]
    for k, cp in enumerate(dg_copies):
        cp.wait_recv()
        total_dg = total_dg + dg_in[k]
    dg_out[...] = total_dg

    for i in range(2):
        for b in range(2):
            out_copy(i, b).wait_send()
            out_copy(i, b).wait_recv()
        for r in (PAIR, NEAR, DIAG):
            in_copy(i, r).wait_send()
    for r in (PAIR, NEAR, DIAG):
        g_copy(r).wait_send()
    for cp in dg_copies:
        cp.wait_send()
    st_copy.wait_send()
    for j in range(CHUNKS):
        for k in range(3):
            for kind in range(7):
                w_copy(kind, k, j).wait_send()
            pair_copy(0, j, k).wait_send()
            pair_copy(1, j, k).wait_send()
            link_copy(j, k).wait_send()


def write_out(*refs):
    n = len(refs) // 2
    copies = [pltpu.make_async_copy(refs[i], refs[n + i], refs[2 * n].at[i]) for i in range(n)]
    for cp in copies:
        cp.start()
    for cp in copies:
        cp.wait()


def solution(mesh):
    def local_step(x_blk, dy_blk, gain_blk, w_gate_blk, w_up_blk, w_down_blk):
        rows, wid = x_blk.shape
        f = w_gate_blk.shape[1]
        tok, d, half, fc = rows // 2, 4 * wid, 2 * wid, f // 8 * max(EIGHTHS)
        vm, dma = pltpu.VMEM, pltpu.SemaphoreType.DMA
        in_vmem = pl.BlockSpec(memory_space=pltpu.VMEM)
        args = (x_blk, dy_blk, gain_blk.reshape(1, wid), w_gate_blk, w_up_blk, w_down_blk)
        outs = pl.pallas_call(
            kernel,
            name="mlp_branch",
            out_shape=(jax.ShapeDtypeStruct((rows, wid), BF16), jax.ShapeDtypeStruct((rows, wid), BF16),
                       jax.ShapeDtypeStruct((wid, f), F32), jax.ShapeDtypeStruct((wid, f), F32),
                       jax.ShapeDtypeStruct((f, wid), F32), jax.ShapeDtypeStruct((1, wid), F32)),
            in_specs=[pl.BlockSpec(memory_space=pltpu.HBM)] * 6,
            out_specs=(in_vmem,) * 6,
            scratch_shapes=[
                vm((tok, d), BF16), vm((tok, d), BF16), vm((4, 1, wid), F32),
                vm((2, d, f), BF16), vm((2, d, f), BF16), vm((2, f, d), BF16),
                vm((tok, d), BF16), vm((half, tok), BF16), vm((half, tok), BF16), vm((tok, d), F32), vm((tok, 1), F32),
                vm((tok, fc), BF16), vm((tok, fc), BF16), vm((tok, fc), BF16),
                vm((2, 2, 3 * wid, f), F32), vm((2, 3 * wid, f), F32), vm((3 * wid, f), F32), vm((3 * wid, f), F32),
                vm((tok, half), F32), vm((tok, half), F32), vm((tok, wid), BF16), vm((tok, half), BF16),
                vm((2, 1, wid), F32), vm((3, 1, wid), F32),
                vm((tok // LN_ROWS, 8, LN_ROWS), F32), vm((tok // LN_ROWS, 8, LN_ROWS), F32),
                dma((4,)), dma((4,)), dma((2, 4)), dma((2, 4)),
                dma((7, 3, CHUNKS)), dma((7, 3, CHUNKS)), dma((2, CHUNKS, 3)), dma((2, CHUNKS, 3)),
                dma((CHUNKS, 3)), dma((CHUNKS, 3)), dma((2, 2)), dma((2, 2)), dma((3,)), dma((3,)), dma(()), dma(()),
                dma((2,)), dma((3, CHUNKS)), dma(()),
            ],
            compiler_params=pltpu.CompilerParams(collective_id=0, has_side_effects=True,
                                                 vmem_limit_bytes=44 * 2 ** 20),
        )(*(pltpu.with_memory_space_constraint(a, pltpu.HBM) for a in args))
        outs = pl.pallas_call(
            write_out,
            name="write_out",
            out_shape=tuple(jax.ShapeDtypeStruct(o.shape, o.dtype) for o in outs),
            in_specs=[in_vmem] * 6,
            out_specs=(pl.BlockSpec(memory_space=pl.ANY),) * 6,
            scratch_shapes=[dma((6,))],
            compiler_params=pltpu.CompilerParams(vmem_limit_bytes=2 ** 20),
        )(*outs)
        return outs[:5] + (outs[5].reshape(wid),)

    return jax.shard_map(
        local_step, mesh=mesh,
        in_specs=(P("ty", "tx"), P("ty", "tx"), P("tx"), P("tx", "ty"), P("tx", "ty"), P("ty", "tx")),
        out_specs=(P("ty", "tx"), P("ty", "tx"), P("tx", "ty"), P("tx", "ty"), P("ty", "tx"), P("tx")),
        check_vma=False)
```

```python
import jax
import jax.numpy as jnp
from jax import lax
from jax.experimental import pallas as pl
from jax.experimental.pallas import tpu as pltpu
from jax.sharding import PartitionSpec as P

LN_EPS = 1e-6
MESH = pl.DeviceIdType.MESH
F32 = jnp.float32
BF16 = jnp.bfloat16

OWN, PAIR, NEAR, DIAG = 0, 1, 2, 3
EIGHTHS = (2, 2, 2, 2)
CHUNKS = len(EIGHTHS)
LN_ROWS = 128
ROW_TILE = 256


def dot(a, b):
    return lax.dot_general(a, b, (((1,), (0,)), ((), ())), preferred_element_type=F32)


def dot_nt(a, b):
    return lax.dot_general(a, b, (((1,), (1,)), ((), ())), preferred_element_type=F32)


def kernel(x_in, dy_in, g_in, w1_in, w3_in, w2_in,
           y_out, dx_out, dw1_out, dw3_out, dw2_out, dg_out,
           xg, dyg, gg, w1g, w3g, w2g, h, h_t, dy_t, xhat, inv_std, act, du, dv, part, pair_in, summed, link_in,
           m_acc, dh_acc, y_st, dx_st, dg_st, dg_in, st_own, st_in,
           g_send, g_recv, in_send, in_recv, w_send, w_recv, dw_send, dw_recv,
           lk_send, lk_recv, out_send, out_recv, dg_send, dg_recv, st_send, st_recv, lc_in, lc_w, lc_g):
    y, t = lax.axis_index("ty"), lax.axis_index("tx")
    x, c = t // 2, t % 2
    tok = x_in.shape[0] // 2
    wid = x_in.shape[1]
    d = 4 * wid
    half = 2 * wid
    unit = w1_in.shape[1] // 8
    size = [e * unit for e in EIGHTHS]
    start = [sum(size[:i]) for i in range(CHUNKS)]
    span = [pl.ds(start[i], size[i]) for i in range(CHUNKS)]
    peer_t = (t, 2 * x + 1 - c, 2 * (1 - x) + c, 2 * (1 - x) + 1 - c)
    peer_c = (c, 1 - c, c, 1 - c)
    dev = {r: (y, peer_t[r]) for r in (PAIR, NEAR, DIAG)}
    cross, cross_pair = (1 - y, t), (1 - y, peer_t[PAIR])

    barrier = pltpu.get_barrier_semaphore()
    for to in (dev[PAIR], dev[NEAR], dev[DIAG], cross, cross_pair):
        pl.semaphore_signal(barrier, inc=1, device_id=to, device_id_type=MESH)
    pl.semaphore_wait(barrier, 5)

    def remote(src, dst, send, recv, to):
        return pltpu.make_async_remote_copy(src_ref=src, dst_ref=dst, send_sem=send, recv_sem=recv,
                                            device_id=to, device_id_type=MESH)

    def col(r):
        return pl.ds(pl.multiple_of(peer_t[r] * wid, wid), wid)

    def rows_of(core):
        return pl.ds(pl.multiple_of(core * tok, tok), tok)

    def core_cols(core):
        return pl.ds(pl.multiple_of(core * wid, wid), wid)

    chip = pl.ds(pl.multiple_of(x * half, half), half)
    tin, tg = (x_in, dy_in), (xg, dyg)

    def in_copy(i, r):
        return remote(tin[i].at[rows_of(peer_c[r]), :], tg[i].at[:, col(OWN)], in_send.at[i, r], in_recv.at[i, r], dev[r])

    def own_copy(i):
        return pltpu.make_async_copy(tin[i].at[rows_of(c), :], tg[i].at[:, col(OWN)], lc_in.at[i])

    def g_copy(r):
        return remote(g_in, gg.at[t], g_send.at[r], g_recv.at[r], dev[r])

    def w_src(w, j):
        if w == 2:
            return w2_in.at[span[j], :]
        return (w1_in, w3_in)[w].at[:, span[j]]

    def w_dst(w, side, j, r):
        if w == 2:
            return w2g.at[side, span[j], col(r)]
        return (w1g, w3g)[w].at[side, col(r), span[j]]

    def w_copy(kind, w, j):
        if kind == 0:
            src, dst, to = w_src(w, j), w_dst(w, 0, j, OWN), dev[NEAR]
        elif kind == 1:
            src, dst, to = w_src(w, j), w_dst(w, 0, j, OWN), dev[PAIR]
        elif kind == 2:
            src, dst, to = w_dst(w, 0, j, NEAR), w_dst(w, 0, j, NEAR), dev[PAIR]
        elif kind == 3:
            src, dst, to = w_src(w, j), w_dst(w, 1, j, OWN), cross
        elif kind == 4:
            src, dst, to = w_dst(w, 1, j, OWN), w_dst(w, 1, j, OWN), dev[NEAR]
        elif kind == 5:
            src, dst, to = w_dst(w, 1, j, OWN), w_dst(w, 1, j, OWN), dev[PAIR]
        else:
            src, dst, to = w_dst(w, 1, j, NEAR), w_dst(w, 1, j, NEAR), dev[PAIR]
        return remote(src, dst, w_send.at[kind], w_recv.at[kind, j], to)

    def w_arrived(kind, j):
        ref = w1g.at[kind // 3 % 2, pl.ds(0, 3 * wid), span[j]]
        pltpu.make_async_copy(ref, ref, w_recv.at[kind, j]).wait()

    def w_sent(kind):
        ref = w1g.at[0, pl.ds(0, 3 * wid), :]
        pltpu.make_async_copy(ref, ref, w_send.at[kind]).wait()

    def own_w(w, j):
        return pltpu.make_async_copy(w_src(w, j), w_dst(w, 0, j, OWN), lc_w)

    for r in (PAIR, NEAR, DIAG):
        g_copy(r).start()
    for i in range(2):
        for r in (NEAR, DIAG):
            in_copy(i, r).start()
    for j in range(CHUNKS):
        for w in range(3):
            w_copy(3, w, j).start()
    for i in range(2):
        in_copy(i, PAIR).start()
        own_copy(i).start()
    own_g = pltpu.make_async_copy(g_in, gg.at[t], lc_g)
    own_g.start()
    for j in range(CHUNKS):
        for w in range(3):
            w_copy(1, w, j).start()
            own_w(w, j).start()

    def pass_cross(j):
        w_arrived(3, j)
        for w in range(3):
            w_copy(4, w, j).start()
            w_copy(5, w, j).start()

    pass_cross(0)
    pass_cross(1)
    own_copy(0).wait()
    own_g.wait()
    for r in (PAIR, NEAR, DIAG):
        in_copy(0, r).wait_recv()
        g_copy(r).wait_recv()
    gain = jnp.concatenate([gg[k] for k in range(4)], axis=1)
    gain_chip = jnp.concatenate([gg[2 * x], gg[2 * x + 1]], axis=1)

    def blocks(n, body, carry=0, lo=0, hi=None):
        def step(k, carry):
            return body(k, pl.ds(pl.multiple_of(k * n, n), n), carry)
        return lax.fori_loop(lo // n, (tok if hi is None else hi) // n, step, carry, unroll=True)

    def ln_rows(k, rows, carry):
        xf = xg[rows, :].astype(F32)
        mu = jnp.sum(xf, axis=1, keepdims=True) * (1.0 / d)
        s = jnp.sum(xf * xf, axis=1, keepdims=True) * (1.0 / d)
        inv = lax.rsqrt(s - mu * mu + LN_EPS)
        xh = (xf - mu) * inv
        xhat[rows, :] = xh
        inv_std[rows, :] = inv
        h[rows, :] = (gain * xh).astype(BF16)
        h_t[:, rows] = h[rows, chip].astype(F32).T.astype(BF16)
        return carry

    def dy_rows(k, rows, carry):
        dy_t[:, rows] = dyg[rows, chip].astype(F32).T.astype(BF16)
        return carry

    blocks(LN_ROWS, ln_rows)
    for j in range(2, CHUNKS):
        pass_cross(j)
    for j in range(CHUNKS):
        for w in range(3):
            w_copy(0, w, j).start()
    own_copy(1).wait()
    for r in (PAIR, NEAR, DIAG):
        in_copy(1, r).wait_recv()
    blocks(LN_ROWS, dy_rows)

    def gated(s, j):
        n = size[j]

        def body(k, rows, carry):
            hr = h[rows, :]
            u = dot(hr, w1g[s, :, span[j]])
            v = dot(hr, w3g[s, :, span[j]])
            da = dot_nt(dyg[rows, :], w2g[s, span[j], :])
            sig = 1.0 / (1.0 + jnp.exp(-u))
            swish = u * sig
            act[rows, :n] = (swish * v).astype(BF16)
            du[rows, :n] = (da * v * sig * (1.0 + u * (1.0 - sig))).astype(BF16)
            dv[rows, :n] = (da * swish).astype(BF16)
            return carry
        blocks(ROW_TILE, body)

    def pair_copy(s, j):
        return remote(part.at[s, 1 - c, :, span[j]], pair_in.at[s, :, span[j]], dw_send.at[s, j], dw_recv.at[s, j], dev[PAIR])

    def weight_grads(s, j):
        for k, (left, right) in enumerate(((h_t, du), (h_t, dv), (dy_t, act))):
            full = dot(left[...], right[:, :size[j]])
            for b in range(2):
                part[s, b, k * wid:(k + 1) * wid, span[j]] = full[b * wid:(b + 1) * wid, :]

    def link_copy(j):
        return remote(summed.at[:, span[j]], link_in.at[:, span[j]], lk_send.at[j], lk_recv.at[j], cross)

    def send_sums(j):
        pair_copy(1, j).wait_recv()
        summed[:, span[j]] = part[1, c, :, span[j]] + pair_in[1, :, span[j]]
        link_copy(j).start()

    def token_sums(s, j, rows):
        n = size[j]
        m = dot(act[rows, :n], w2g[s, span[j], chip])
        dh = dot_nt(du[rows, :n], w1g[s, chip, span[j]]) + dot_nt(dv[rows, :n], w3g[s, chip, span[j]])
        return m, dh

    def to_tokens(s, j, first=False):
        def body(k, rows, carry):
            m, dh = token_sums(s, j, rows)
            if first:
                m_acc[rows, :] = m
                dh_acc[rows, :] = dh
            else:
                m_acc[rows, :] += m
                dh_acc[rows, :] += dh
            return carry
        blocks(ROW_TILE, body)

    def pass_near(kind, j):
        w_arrived(kind, j)
        for w in range(3):
            w_copy(6 if kind == 4 else 2, w, j).start()

    pass_near(4, 0)
    for j in range(CHUNKS):
        w_arrived(5, j)
        w_arrived(6, j)
        if j > 1:
            send_sums(j - 1)
        gated(1, j)
        weight_grads(1, j)
        if j == 0:
            pair_copy(1, j).start()
        to_tokens(1, j, first=j == 0)
        if j:
            pair_copy(1, j).start()
        if j == 0:
            send_sums(j)
        if j + 1 < CHUNKS:
            pass_near(4, j + 1)
        else:
            pass_near(0, 0)

    def finish_dw(j):
        pair_copy(0, j).wait_recv()
        link_copy(j).wait_recv()
        for k in range(3):
            band = pl.ds(k * wid, wid)
            total = part[0, c, band, span[j]] + pair_in[0, band, span[j]] + link_in[band, span[j]]
            if k == 2:
                dw2_out[span[j], :] = total.T
            else:
                (dw1_out, dw3_out)[k][:, span[j]] = total

    lane = lax.broadcasted_iota(jnp.int32, (LN_ROWS, LN_ROWS), 1)
    last = CHUNKS - 1

    def last_rows(k, rows, dg):
        m, dh = token_sums(0, last, rows)
        m_acc[rows, :] += m
        dh = dh_acc[rows, :] + dh
        dh_acc[rows, :] = dh
        xh = xhat[rows, chip]
        e = dh * gain_chip
        se = jnp.sum(e, axis=1, keepdims=True)
        sex = jnp.sum(e * xh, axis=1, keepdims=True)
        st_own[k] = jnp.where(lane == 0, se, jnp.where(lane == 1, sex, 0.0)).T[:8, :]
        return dg + jnp.sum(dh * xh, axis=0, keepdims=True)

    for j in range(CHUNKS):
        w_arrived(1, j)
        w_arrived(2, j)
        if j == 0:
            send_sums(last)
            ref = w1g.at[0, pl.ds(0, 3 * wid), :]
            pltpu.make_async_copy(ref, ref, lc_w).wait()
        gated(0, j)
        if j < last:
            weight_grads(0, j)
            to_tokens(0, j)
            pair_copy(0, j).start()
            pass_near(0, j + 1)
            if j:
                finish_dw(j - 1)

    dg = blocks(LN_ROWS, last_rows, jnp.zeros((1, half), F32))
    st_copy = remote(st_own, st_in, st_send, st_recv, dev[NEAR])
    st_copy.start()
    weight_grads(0, last)
    pair_copy(0, last).start()

    outs, stage = (y_out, dx_out), (y_st, dx_st)
    mid = tok // 2

    def out_copy(i, part_of):
        rows = pl.ds(part_of * mid, mid)
        to_rows = pl.ds(pl.multiple_of(c * tok + part_of * mid, mid), mid)
        src = y_st.at[rows, :] if i == 0 else dx_st.at[rows, core_cols(1 - c)]
        return remote(src, outs[i].at[to_rows, :], out_send.at[i, part_of], out_recv.at[i, part_of], dev[PAIR])

    def out_rows(k):
        return pl.ds(pl.multiple_of(c * tok + k * LN_ROWS, LN_ROWS), LN_ROWS)

    def y_rows(k, rows, carry):
        y_st[rows, :] = (xg[rows, col(PAIR)].astype(F32) + m_acc[rows, core_cols(1 - c)]).astype(BF16)
        y_out[out_rows(k), :] = (xg[rows, col(OWN)].astype(F32) + m_acc[rows, core_cols(c)]).astype(BF16)
        return carry

    blocks(LN_ROWS, y_rows)
    for b in range(2):
        dg_st[b] = dg[:, b * wid:(b + 1) * wid]
        out_copy(0, b).start()
    dg_copies = [remote(dg_st.at[b], dg_in.at[k], dg_send.at[k], dg_recv.at[k], to)
                 for k, (b, to) in enumerate(((1 - c, dev[PAIR]), (c, cross), (1 - c, cross_pair)))]
    for cp in dg_copies:
        cp.start()

    for r in (PAIR, NEAR, DIAG):
        g_copy(r).wait_send()
        for i in range(2):
            in_copy(i, r).wait_send()
    for kind in range(7):
        w_sent(kind)
    for j in range(CHUNKS):
        pair_copy(1, j).wait_send()
        if j < last:
            pair_copy(0, j).wait_send()
        if j < last - 1:
            link_copy(j).wait_send()
    st_copy.wait_recv()

    def dx_rows(k, rows, carry):
        both = jnp.concatenate([st_own[k] + st_in[k], jnp.zeros((LN_ROWS - 8, LN_ROWS), F32)], axis=0).T * (1.0 / d)
        e = dh_acc[rows, :] * gain_chip
        dx_ln = inv_std[rows, :] * (e - both[:, 0:1] - xhat[rows, chip] * both[:, 1:2])
        dx_st[rows, :] = (dyg[rows, chip].astype(F32) + dx_ln).astype(BF16)
        dx_out[out_rows(k), :] = dx_st[rows, core_cols(c)]
        return carry

    for b in range(2):
        blocks(LN_ROWS, dx_rows, lo=b * mid, hi=(b + 1) * mid)
        out_copy(1, b).start()

    finish_dw(last - 1)
    finish_dw(last)

    total_dg = dg_st[c]
    for k, cp in enumerate(dg_copies):
        cp.wait_recv()
        total_dg = total_dg + dg_in[k]
    dg_out[...] = total_dg

    for i in range(2):
        for b in range(2):
            out_copy(i, b).wait_send()
            out_copy(i, b).wait_recv()
    for cp in dg_copies:
        cp.wait_send()
    st_copy.wait_send()
    pair_copy(0, last).wait_send()
    link_copy(last - 1).wait_send()
    link_copy(last).wait_send()


def write_out(*refs):
    n = len(refs) // 2
    copies = [pltpu.make_async_copy(refs[i], refs[n + i], refs[2 * n].at[i]) for i in range(n)]
    for cp in copies:
        cp.start()
    for cp in copies:
        cp.wait()


def solution(mesh):
    def local_step(x_blk, dy_blk, gain_blk, w_gate_blk, w_up_blk, w_down_blk):
        rows, wid = x_blk.shape
        f = w_gate_blk.shape[1]
        tok, d, half, fc = rows // 2, 4 * wid, 2 * wid, f // 8 * max(EIGHTHS)
        vm, dma = pltpu.VMEM, pltpu.SemaphoreType.DMA
        in_vmem = pl.BlockSpec(memory_space=pltpu.VMEM)
        args = (x_blk, dy_blk, gain_blk.reshape(1, wid), w_gate_blk, w_up_blk, w_down_blk)
        outs = pl.pallas_call(
            kernel,
            name="mlp_branch",
            out_shape=(jax.ShapeDtypeStruct((rows, wid), BF16), jax.ShapeDtypeStruct((rows, wid), BF16),
                       jax.ShapeDtypeStruct((wid, f), F32), jax.ShapeDtypeStruct((wid, f), F32),
                       jax.ShapeDtypeStruct((f, wid), F32), jax.ShapeDtypeStruct((1, wid), F32)),
            in_specs=[pl.BlockSpec(memory_space=pltpu.HBM)] * 6,
            out_specs=(in_vmem,) * 6,
            scratch_shapes=[
                vm((tok, d), BF16), vm((tok, d), BF16), vm((4, 1, wid), F32),
                vm((2, d, f), BF16), vm((2, d, f), BF16), vm((2, f, d), BF16),
                vm((tok, d), BF16), vm((half, tok), BF16), vm((half, tok), BF16), vm((tok, d), F32), vm((tok, 1), F32),
                vm((tok, fc), BF16), vm((tok, fc), BF16), vm((tok, fc), BF16),
                vm((2, 2, 3 * wid, f), F32), vm((2, 3 * wid, f), F32), vm((3 * wid, f), F32), vm((3 * wid, f), F32),
                vm((tok, half), F32), vm((tok, half), F32), vm((tok, wid), BF16), vm((tok, half), BF16),
                vm((2, 1, wid), F32), vm((3, 1, wid), F32),
                vm((tok // LN_ROWS, 8, LN_ROWS), F32), vm((tok // LN_ROWS, 8, LN_ROWS), F32),
                dma((4,)), dma((4,)), dma((2, 4)), dma((2, 4)),
                dma((7,)), dma((7, CHUNKS)), dma((2, CHUNKS)), dma((2, CHUNKS)),
                dma((CHUNKS,)), dma((CHUNKS,)), dma((2, 2)), dma((2, 2)), dma((3,)), dma((3,)), dma(()), dma(()),
                dma((2,)), dma(()), dma(()),
            ],
            compiler_params=pltpu.CompilerParams(collective_id=0, has_side_effects=True,
                                                 vmem_limit_bytes=44 * 2 ** 20),
        )(*(pltpu.with_memory_space_constraint(a, pltpu.HBM) for a in args))
        outs = pl.pallas_call(
            write_out,
            name="write_out",
            out_shape=tuple(jax.ShapeDtypeStruct(o.shape, o.dtype) for o in outs),
            in_specs=[in_vmem] * 6,
            out_specs=(pl.BlockSpec(memory_space=pl.ANY),) * 6,
            scratch_shapes=[dma((6,))],
            compiler_params=pltpu.CompilerParams(vmem_limit_bytes=2 ** 20),
        )(*outs)
        return outs[:5] + (outs[5].reshape(wid),)

    return jax.shard_map(
        local_step, mesh=mesh,
        in_specs=(P("ty", "tx"), P("ty", "tx"), P("tx"), P("tx", "ty"), P("tx", "ty"), P("ty", "tx")),
        out_specs=(P("ty", "tx"), P("ty", "tx"), P("tx", "ty"), P("tx", "ty"), P("ty", "tx"), P("tx")),
        check_vma=False)
```

```python
import jax
import jax.numpy as jnp
from jax import lax
from jax.experimental import pallas as pl
from jax.experimental.pallas import tpu as pltpu
from jax.sharding import PartitionSpec as P

LN_EPS = 1e-6
MESH = pl.DeviceIdType.MESH
F32 = jnp.float32
BF16 = jnp.bfloat16

OWN, PAIR, NEAR, DIAG = 0, 1, 2, 3
EIGHTHS = (2, 2, 2, 2)
CHUNKS = len(EIGHTHS)
LN_ROWS = 128
ROW_TILE = 256


def dot(a, b):
    return lax.dot_general(a, b, (((1,), (0,)), ((), ())), preferred_element_type=F32)


def dot_nt(a, b):
    return lax.dot_general(a, b, (((1,), (1,)), ((), ())), preferred_element_type=F32)


def kernel(x_in, dy_in, g_in, w1_in, w3_in, w2_in,
           y_out, dx_out, dw1_out, dw3_out, dw2_out, dg_out,
           xg, dyg, gg, w1g, w3g, w2g, h, h_t, dy_t, xhat, inv_std, act, du, dv, part, pair_in, summed, link_in,
           m_acc, dh_acc, dh_last, y_st, dx_st, dg_st, dg_in, st_own, st_in,
           g_send, g_recv, in_send, in_recv, w_send, w_recv, dw_send, dw_recv,
           lk_send, lk_recv, out_send, out_recv, dg_send, dg_recv, st_send, st_recv, lc_in, lc_w, lc_g):
    y, t = lax.axis_index("ty"), lax.axis_index("tx")
    x, c = t // 2, t % 2
    tok = x_in.shape[0] // 2
    wid = x_in.shape[1]
    d = 4 * wid
    half = 2 * wid
    unit = w1_in.shape[1] // 8
    size = [e * unit for e in EIGHTHS]
    start = [sum(size[:i]) for i in range(CHUNKS)]
    span = [pl.ds(start[i], size[i]) for i in range(CHUNKS)]
    peer_t = (t, 2 * x + 1 - c, 2 * (1 - x) + c, 2 * (1 - x) + 1 - c)
    peer_c = (c, 1 - c, c, 1 - c)
    dev = {r: (y, peer_t[r]) for r in (PAIR, NEAR, DIAG)}
    cross, cross_pair = (1 - y, t), (1 - y, peer_t[PAIR])

    barrier = pltpu.get_barrier_semaphore()
    for to in (dev[PAIR], dev[NEAR], dev[DIAG], cross, cross_pair):
        pl.semaphore_signal(barrier, inc=1, device_id=to, device_id_type=MESH)
    pl.semaphore_wait(barrier, 5)

    def remote(src, dst, send, recv, to):
        return pltpu.make_async_remote_copy(src_ref=src, dst_ref=dst, send_sem=send, recv_sem=recv,
                                            device_id=to, device_id_type=MESH)

    def col(r):
        return pl.ds(pl.multiple_of(peer_t[r] * wid, wid), wid)

    def rows_of(core):
        return pl.ds(pl.multiple_of(core * tok, tok), tok)

    def core_cols(core):
        return pl.ds(pl.multiple_of(core * wid, wid), wid)

    chip = pl.ds(pl.multiple_of(x * half, half), half)
    tin, tg = (x_in, dy_in), (xg, dyg)

    def in_copy(i, r):
        return remote(tin[i].at[rows_of(peer_c[r]), :], tg[i].at[:, col(OWN)], in_send.at[i, r], in_recv.at[i, r], dev[r])

    def own_copy(i):
        return pltpu.make_async_copy(tin[i].at[rows_of(c), :], tg[i].at[:, col(OWN)], lc_in.at[i])

    def g_copy(r):
        return remote(g_in, gg.at[t], g_send.at[r], g_recv.at[r], dev[r])

    def w_src(w, j):
        if w == 2:
            return w2_in.at[span[j], :]
        return (w1_in, w3_in)[w].at[:, span[j]]

    def w_dst(w, side, j, r):
        if w == 2:
            return w2g.at[side, span[j], col(r)]
        return (w1g, w3g)[w].at[side, col(r), span[j]]

    def w_copy(kind, w, j):
        if kind == 0:
            src, dst, to = w_src(w, j), w_dst(w, 0, j, OWN), dev[NEAR]
        elif kind == 1:
            src, dst, to = w_src(w, j), w_dst(w, 0, j, OWN), dev[PAIR]
        elif kind == 2:
            src, dst, to = w_dst(w, 0, j, NEAR), w_dst(w, 0, j, NEAR), dev[PAIR]
        elif kind == 3:
            src, dst, to = w_src(w, j), w_dst(w, 1, j, OWN), cross
        elif kind == 4:
            src, dst, to = w_dst(w, 1, j, OWN), w_dst(w, 1, j, OWN), dev[NEAR]
        elif kind == 5:
            src, dst, to = w_dst(w, 1, j, OWN), w_dst(w, 1, j, OWN), dev[PAIR]
        else:
            src, dst, to = w_dst(w, 1, j, NEAR), w_dst(w, 1, j, NEAR), dev[PAIR]
        slot = CHUNKS if w == 2 and j == 0 and kind in (4, 6) else j
        return remote(src, dst, w_send.at[kind], w_recv.at[kind, slot], to)

    def w_arrived(kind, j, n=3, slot=None):
        ref = w1g.at[0 if kind < 3 else 1, pl.ds(0, n * wid), span[j]]
        pltpu.make_async_copy(ref, ref, w_recv.at[kind, j if slot is None else slot]).wait()

    def w_sent(kind):
        ref = w1g.at[0, pl.ds(0, 3 * wid), :]
        pltpu.make_async_copy(ref, ref, w_send.at[kind]).wait()

    def own_w(w, j):
        return pltpu.make_async_copy(w_src(w, j), w_dst(w, 0, j, OWN), lc_w)

    for r in (PAIR, NEAR, DIAG):
        g_copy(r).start()
    for r in (NEAR, DIAG):
        in_copy(0, r).start()
    for j in range(CHUNKS):
        for w in range(3):
            w_copy(3, w, j).start()
    for i in range(2):
        in_copy(i, PAIR).start()
        own_copy(i).start()
    own_g = pltpu.make_async_copy(g_in, gg.at[t], lc_g)
    own_g.start()
    for j in range(CHUNKS):
        for w in range(3):
            w_copy(1, w, j).start()
            own_w(w, j).start()

    def pass_cross(j):
        w_arrived(3, j)
        for w in range(3):
            if j == 0 and w == 2:
                for r in (NEAR, DIAG):
                    in_copy(1, r).start()
            w_copy(4, w, j).start()
        for w in range(3):
            w_copy(5, w, j).start()

    pass_cross(0)
    pass_cross(1)
    own_copy(0).wait()
    own_g.wait()
    for r in (PAIR, NEAR, DIAG):
        in_copy(0, r).wait_recv()
        g_copy(r).wait_recv()
    gain = jnp.concatenate([gg[k] for k in range(4)], axis=1)
    gain_chip = jnp.concatenate([gg[2 * x], gg[2 * x + 1]], axis=1)

    def blocks(n, body, carry=0, lo=0, hi=None):
        def step(k, carry):
            return body(k, pl.ds(pl.multiple_of(k * n, n), n), carry)
        return lax.fori_loop(lo // n, (tok if hi is None else hi) // n, step, carry, unroll=True)

    def ln_rows(k, rows, carry):
        xf = xg[rows, :].astype(F32)
        mu = jnp.sum(xf, axis=1, keepdims=True) * (1.0 / d)
        s = jnp.sum(xf * xf, axis=1, keepdims=True) * (1.0 / d)
        inv = lax.rsqrt(s - mu * mu + LN_EPS)
        xh = (xf - mu) * inv
        xhat[rows, :] = xh
        inv_std[rows, :] = inv
        h[rows, :] = (gain * xh).astype(BF16)
        h_t[:, rows] = h[rows, chip].astype(F32).T.astype(BF16)
        return carry

    def dy_rows(k, rows, carry):
        dy_t[:, rows] = dyg[rows, chip].astype(F32).T.astype(BF16)
        return carry

    def early_act(k, rows, carry):
        hr = h[rows, :]
        u = dot(hr, w1g[1, :, span[0]])
        v = dot(hr, w3g[1, :, span[0]])
        act[rows, :size[0]] = (u * (1.0 / (1.0 + jnp.exp(-u))) * v).astype(BF16)
        return carry

    def gated(s, j):
        n = size[j]

        def body(k, rows, carry):
            hr = h[rows, :]
            u = dot(hr, w1g[s, :, span[j]])
            v = dot(hr, w3g[s, :, span[j]])
            da = dot_nt(dyg[rows, :], w2g[s, span[j], :])
            sig = 1.0 / (1.0 + jnp.exp(-u))
            swish = u * sig
            act[rows, :n] = (swish * v).astype(BF16)
            du[rows, :n] = (da * v * sig * (1.0 + u * (1.0 - sig))).astype(BF16)
            dv[rows, :n] = (da * swish).astype(BF16)
            return carry
        blocks(ROW_TILE, body)

    EARLY, LATE = (2, 3, CHUNKS), (0, 2, 0)

    def bands(j, piece):
        lo, hi, slot = piece or (0, 3, j)
        return pl.ds(lo * wid, (hi - lo) * wid), slot

    def pair_copy(s, j, piece=None):
        band, slot = bands(j, piece)
        return remote(part.at[s, 1 - c, band, span[j]], pair_in.at[s, band, span[j]],
                      dw_send.at[s, slot], dw_recv.at[s, slot], dev[PAIR])

    def weight_grads(s, j, lo=0, hi=3):
        for k, (left, right) in tuple(enumerate(((h_t, du), (h_t, dv), (dy_t, act))))[lo:hi]:
            full = dot(left[...], right[:, :size[j]])
            for b in range(2):
                part[s, b, k * wid:(k + 1) * wid, span[j]] = full[b * wid:(b + 1) * wid, :]

    def link_copy(j, piece=None):
        band, slot = bands(j, piece)
        return remote(summed.at[band, span[j]], link_in.at[band, span[j]], lk_send.at[slot], lk_recv.at[slot], cross)

    def send_sums(j, piece=None):
        band, _ = bands(j, piece)
        pair_copy(1, j, piece).wait_recv()
        summed[band, span[j]] = part[1, c, band, span[j]] + pair_in[1, band, span[j]]
        link_copy(j, piece).start()

    def token_sums(s, j, rows):
        n = size[j]
        m = dot(act[rows, :n], w2g[s, span[j], chip])
        dh = dot_nt(du[rows, :n], w1g[s, chip, span[j]]) + dot_nt(dv[rows, :n], w3g[s, chip, span[j]])
        return m, dh

    def to_tokens(s, j, first=False):
        def body(k, rows, carry):
            m, dh = token_sums(s, j, rows)
            if first:
                m_acc[rows, :] = m
                dh_acc[rows, :] = dh
            else:
                m_acc[rows, :] += m
                dh_acc[rows, :] += dh
            return carry
        blocks(ROW_TILE, body)

    def pass_near(kind, j):
        w_arrived(kind, j)
        for w in range(3):
            w_copy(6 if kind == 4 else 2, w, j).start()

    blocks(LN_ROWS, ln_rows)
    own_copy(1).wait()
    in_copy(1, PAIR).wait_recv()
    blocks(LN_ROWS, dy_rows)
    pass_cross(2)
    w_arrived(4, 0, 2)
    for w in range(2):
        w_copy(6, w, 0).start()
    w_arrived(5, 0)
    w_arrived(6, 0, 2)
    blocks(ROW_TILE, early_act)
    weight_grads(1, 0, 2, 3)
    pair_copy(1, 0, EARLY).start()
    for j in range(3, CHUNKS):
        pass_cross(j)
    for j in range(CHUNKS):
        for w in range(3):
            w_copy(0, w, j).start()
    send_sums(0, EARLY)
    for r in (NEAR, DIAG):
        in_copy(1, r).wait_recv()

    w_arrived(4, 0, 1, CHUNKS)
    w_copy(6, 2, 0).start()
    for j in range(CHUNKS):
        if j:
            w_arrived(5, j)
            w_arrived(6, j)
        else:
            w_arrived(6, 0, 1, CHUNKS)
        if j > 1:
            send_sums(j - 1)
        gated(1, j)
        weight_grads(1, j, 0, 3 if j else 2)
        if j == 0:
            pair_copy(1, j, LATE).start()
        to_tokens(1, j, first=j == 0)
        if j:
            pair_copy(1, j).start()
        if j == 0:
            send_sums(j, LATE)
        if j + 1 < CHUNKS:
            pass_near(4, j + 1)
        else:
            pass_near(0, 0)

    def finish_dw(j):
        pair_copy(0, j).wait_recv()
        for piece in (EARLY, LATE) if j == 0 else (None,):
            link_copy(j, piece).wait_recv()
        for k in range(3):
            band = pl.ds(k * wid, wid)
            total = part[0, c, band, span[j]] + pair_in[0, band, span[j]] + link_in[band, span[j]]
            if k == 2:
                dw2_out[span[j], :] = total.T
            else:
                (dw1_out, dw3_out)[k][:, span[j]] = total

    lane = lax.broadcasted_iota(jnp.int32, (LN_ROWS, LN_ROWS), 1)
    last = CHUNKS - 1

    def sum_rows(k, rows, carry):
        e = dh_acc[rows, :] * gain_chip
        se = jnp.sum(e, axis=1, keepdims=True)
        sex = jnp.sum(e * xhat[rows, chip], axis=1, keepdims=True)
        st_own[k] = jnp.where(lane == 0, se, jnp.where(lane == 1, sex, 0.0)).T[:8, :]
        return carry

    st_copy = remote(st_own, st_in, st_send, st_recv, dev[NEAR])
    for j in range(CHUNKS):
        w_arrived(1, j)
        w_arrived(2, j)
        if j == 0:
            send_sums(last)
            ref = w1g.at[0, pl.ds(0, 3 * wid), :]
            pltpu.make_async_copy(ref, ref, lc_w).wait()
        gated(0, j)
        weight_grads(0, j)
        if j < last:
            to_tokens(0, j)
            pair_copy(0, j).start()
            if j == last - 1:
                blocks(LN_ROWS, sum_rows)
                st_copy.start()
            pass_near(0, j + 1)
            if j:
                finish_dw(j - 1)
    pair_copy(0, last).start()
    st_copy.wait_recv()

    outs, stage = (y_out, dx_out), (y_st, dx_st)
    mid = tok // 2

    def out_copy(i, part_of):
        rows = pl.ds(part_of * mid, mid)
        to_rows = pl.ds(pl.multiple_of(c * tok + part_of * mid, mid), mid)
        return remote(stage[i].at[rows, core_cols(1 - c)], outs[i].at[to_rows, :],
                      out_send.at[i, part_of], out_recv.at[i, part_of], dev[PAIR])

    def out_rows(k):
        return pl.ds(pl.multiple_of(c * tok + k * LN_ROWS, LN_ROWS), LN_ROWS)

    def last_rows(k, rows, dg):
        n = size[last]
        m = dot(act[rows, :n], w2g[0, span[last], chip])
        full = dot_nt(du[rows, :n], w1g[0, :, span[last]]) + dot_nt(dv[rows, :n], w3g[0, :, span[last]])
        dh_last[rows, :] = full
        e = full * gain
        before = jnp.concatenate([st_own[k] + st_in[k], jnp.zeros((LN_ROWS - 8, LN_ROWS), F32)], axis=0).T
        me = (before[:, 0:1] + jnp.sum(e, axis=1, keepdims=True)) * (1.0 / d)
        mex = (before[:, 1:2] + jnp.sum(e * xhat[rows, :], axis=1, keepdims=True)) * (1.0 / d)
        dh = dh_acc[rows, :] + dh_last[rows, chip]
        xh = xhat[rows, chip]
        dx_ln = inv_std[rows, :] * (dh * gain_chip - me - xh * mex)
        dx_st[rows, :] = (dyg[rows, chip].astype(F32) + dx_ln).astype(BF16)
        dx_out[out_rows(k), :] = dx_st[rows, core_cols(c)]
        y_st[rows, :] = (xg[rows, chip].astype(F32) + (m_acc[rows, :] + m)).astype(BF16)
        y_out[out_rows(k), :] = y_st[rows, core_cols(c)]
        return dg + jnp.sum(dh * xh, axis=0, keepdims=True)

    dg = jnp.zeros((1, half), F32)
    for b in range(2):
        dg = blocks(LN_ROWS, last_rows, dg, lo=b * mid, hi=(b + 1) * mid)
        out_copy(0, b).start()
        out_copy(1, b).start()
    for b in range(2):
        dg_st[b] = dg[:, b * wid:(b + 1) * wid]
    dg_copies = [remote(dg_st.at[b], dg_in.at[k], dg_send.at[k], dg_recv.at[k], to)
                 for k, (b, to) in enumerate(((1 - c, dev[PAIR]), (c, cross), (1 - c, cross_pair)))]
    for cp in dg_copies:
        cp.start()

    for r in (PAIR, NEAR, DIAG):
        g_copy(r).wait_send()
        for i in range(2):
            in_copy(i, r).wait_send()
    for kind in range(7):
        w_sent(kind)
    st_copy.wait_send()
    for j in range(CHUNKS):
        pair_copy(0, j).wait_send()
        for piece in (EARLY, LATE) if j == 0 else (None,):
            pair_copy(1, j, piece).wait_send()
            if j < last - 1:
                link_copy(j, piece).wait_send()

    finish_dw(last - 1)
    finish_dw(last)

    total_dg = dg_st[c]
    for k, cp in enumerate(dg_copies):
        cp.wait_recv()
        total_dg = total_dg + dg_in[k]
    dg_out[...] = total_dg

    for i in range(2):
        for b in range(2):
            out_copy(i, b).wait_send()
            out_copy(i, b).wait_recv()
    for cp in dg_copies:
        cp.wait_send()
    link_copy(last - 1).wait_send()
    link_copy(last).wait_send()


def write_out(*refs):
    n = len(refs) // 2
    copies = [pltpu.make_async_copy(refs[i], refs[n + i], refs[2 * n].at[i]) for i in range(n)]
    for cp in copies:
        cp.start()
    for cp in copies:
        cp.wait()


def solution(mesh):
    def local_step(x_blk, dy_blk, gain_blk, w_gate_blk, w_up_blk, w_down_blk):
        rows, wid = x_blk.shape
        f = w_gate_blk.shape[1]
        tok, d, half, fc = rows // 2, 4 * wid, 2 * wid, f // 8 * max(EIGHTHS)
        vm, dma = pltpu.VMEM, pltpu.SemaphoreType.DMA
        in_vmem = pl.BlockSpec(memory_space=pltpu.VMEM)
        args = (x_blk, dy_blk, gain_blk.reshape(1, wid), w_gate_blk, w_up_blk, w_down_blk)
        outs = pl.pallas_call(
            kernel,
            name="mlp_branch",
            out_shape=(jax.ShapeDtypeStruct((rows, wid), BF16), jax.ShapeDtypeStruct((rows, wid), BF16),
                       jax.ShapeDtypeStruct((wid, f), F32), jax.ShapeDtypeStruct((wid, f), F32),
                       jax.ShapeDtypeStruct((f, wid), F32), jax.ShapeDtypeStruct((1, wid), F32)),
            in_specs=[pl.BlockSpec(memory_space=pltpu.HBM)] * 6,
            out_specs=(in_vmem,) * 6,
            scratch_shapes=[
                vm((tok, d), BF16), vm((tok, d), BF16), vm((4, 1, wid), F32),
                vm((2, d, f), BF16), vm((2, d, f), BF16), vm((2, f, d), BF16),
                vm((tok, d), BF16), vm((half, tok), BF16), vm((half, tok), BF16), vm((tok, d), F32), vm((tok, 1), F32),
                vm((tok, fc), BF16), vm((tok, fc), BF16), vm((tok, fc), BF16),
                vm((2, 2, 3 * wid, f), F32), vm((2, 3 * wid, f), F32), vm((3 * wid, f), F32), vm((3 * wid, f), F32),
                vm((tok, half), F32), vm((tok, half), F32), vm((tok, d), F32), vm((tok, half), BF16), vm((tok, half), BF16),
                vm((2, 1, wid), F32), vm((3, 1, wid), F32),
                vm((tok // LN_ROWS, 8, LN_ROWS), F32), vm((tok // LN_ROWS, 8, LN_ROWS), F32),
                dma((4,)), dma((4,)), dma((2, 4)), dma((2, 4)),
                dma((7,)), dma((7, CHUNKS + 1)), dma((2, CHUNKS + 1)), dma((2, CHUNKS + 1)),
                dma((CHUNKS + 1,)), dma((CHUNKS + 1,)), dma((2, 2)), dma((2, 2)), dma((3,)), dma((3,)), dma(()), dma(()),
                dma((2,)), dma(()), dma(()),
            ],
            compiler_params=pltpu.CompilerParams(collective_id=0, has_side_effects=True,
                                                 vmem_limit_bytes=44 * 2 ** 20),
        )(*(pltpu.with_memory_space_constraint(a, pltpu.HBM) for a in args))
        outs = pl.pallas_call(
            write_out,
            name="write_out",
            out_shape=tuple(jax.ShapeDtypeStruct(o.shape, o.dtype) for o in outs),
            in_specs=[in_vmem] * 6,
            out_specs=(pl.BlockSpec(memory_space=pl.ANY),) * 6,
            scratch_shapes=[dma((6,))],
            compiler_params=pltpu.CompilerParams(vmem_limit_bytes=2 ** 20),
        )(*outs)
        return outs[:5] + (outs[5].reshape(wid),)

    return jax.shard_map(
        local_step, mesh=mesh,
        in_specs=(P("ty", "tx"), P("ty", "tx"), P("tx"), P("tx", "ty"), P("tx", "ty"), P("ty", "tx")),
        out_specs=(P("ty", "tx"), P("ty", "tx"), P("tx", "ty"), P("tx", "ty"), P("ty", "tx"), P("tx")),
        check_vma=False)
```

```python
import jax
import jax.numpy as jnp
from jax import lax
from jax.experimental import pallas as pl
from jax.experimental.pallas import tpu as pltpu
from jax.sharding import PartitionSpec as P

LN_EPS = 1e-6
MESH = pl.DeviceIdType.MESH
F32 = jnp.float32
BF16 = jnp.bfloat16

OWN, PAIR, NEAR, DIAG = 0, 1, 2, 3
EIGHTHS = (2, 2, 2, 2)
CHUNKS = len(EIGHTHS)
LN_ROWS = 128
ROW_TILE = 256


def dot(a, b):
    return lax.dot_general(a, b, (((1,), (0,)), ((), ())), preferred_element_type=F32)


def dot_nt(a, b):
    return lax.dot_general(a, b, (((1,), (1,)), ((), ())), preferred_element_type=F32)


def kernel(x_in, dy_in, g_in, w1_in, w3_in, w2_in,
           y_out, dx_out, dw1_out, dw3_out, dw2_out, dg_out,
           xg, dyg, gg, w1g, w3g, w2g, h, h_t, dy_t, xhat, inv_std, uv, act, du, dv, part, pair_in, summed, link_in,
           m_acc, dh_acc, dh_last, means, y_st, dx_st, dg_st, dg_in, st_own, st_in,
           g_send, g_recv, in_send, in_recv, w_send, w_recv, dw_send, dw_recv,
           lk_send, lk_recv, out_send, out_recv, dg_send, dg_recv, st_send, st_recv, lc_in, lc_w, lc_g):
    y, t = lax.axis_index("ty"), lax.axis_index("tx")
    x, c = t // 2, t % 2
    tok = x_in.shape[0] // 2
    wid = x_in.shape[1]
    d = 4 * wid
    half = 2 * wid
    unit = w1_in.shape[1] // 8
    size = [e * unit for e in EIGHTHS]
    start = [sum(size[:i]) for i in range(CHUNKS)]
    span = [pl.ds(start[i], size[i]) for i in range(CHUNKS)]
    peer_t = (t, 2 * x + 1 - c, 2 * (1 - x) + c, 2 * (1 - x) + 1 - c)
    peer_c = (c, 1 - c, c, 1 - c)
    dev = {r: (y, peer_t[r]) for r in (PAIR, NEAR, DIAG)}
    cross, cross_pair = (1 - y, t), (1 - y, peer_t[PAIR])

    barrier = pltpu.get_barrier_semaphore()
    for to in (dev[PAIR], dev[NEAR], dev[DIAG], cross, cross_pair):
        pl.semaphore_signal(barrier, inc=1, device_id=to, device_id_type=MESH)
    pl.semaphore_wait(barrier, 5)

    def remote(src, dst, send, recv, to):
        return pltpu.make_async_remote_copy(src_ref=src, dst_ref=dst, send_sem=send, recv_sem=recv,
                                            device_id=to, device_id_type=MESH)

    def col(r):
        return pl.ds(pl.multiple_of(peer_t[r] * wid, wid), wid)

    def rows_of(core):
        return pl.ds(pl.multiple_of(core * tok, tok), tok)

    def core_cols(core):
        return pl.ds(pl.multiple_of(core * wid, wid), wid)

    chip = pl.ds(pl.multiple_of(x * half, half), half)
    tin, tg = (x_in, dy_in), (xg, dyg)

    def in_copy(i, r):
        return remote(tin[i].at[rows_of(peer_c[r]), :], tg[i].at[:, col(OWN)], in_send, in_recv.at[i, r - 1], dev[r])

    def own_copy(i):
        return pltpu.make_async_copy(tin[i].at[rows_of(c), :], tg[i].at[:, col(OWN)], lc_in.at[i])

    def g_copy(r):
        return remote(g_in, gg.at[t], g_send, g_recv, dev[r])

    def w_src(w, j):
        if w == 2:
            return w2_in.at[span[j], :]
        return (w1_in, w3_in)[w].at[:, span[j]]

    def w_dst(w, side, j, r):
        if w == 2:
            return w2g.at[side, span[j], col(r)]
        return (w1g, w3g)[w].at[side, col(r), span[j]]

    def w_copy(kind, w, j):
        if kind == 0:
            src, dst, to = w_src(w, j), w_dst(w, 0, j, OWN), dev[NEAR]
        elif kind == 1:
            src, dst, to = w_src(w, j), w_dst(w, 0, j, OWN), dev[PAIR]
        elif kind == 2:
            src, dst, to = w_dst(w, 0, j, NEAR), w_dst(w, 0, j, NEAR), dev[PAIR]
        elif kind == 3:
            src, dst, to = w_src(w, j), w_dst(w, 1, j, OWN), cross
        elif kind == 4:
            src, dst, to = w_dst(w, 1, j, OWN), w_dst(w, 1, j, OWN), dev[NEAR]
        elif kind == 5:
            src, dst, to = w_dst(w, 1, j, OWN), w_dst(w, 1, j, OWN), dev[PAIR]
        else:
            src, dst, to = w_dst(w, 1, j, NEAR), w_dst(w, 1, j, NEAR), dev[PAIR]
        return remote(src, dst, w_send.at[kind // 4], w_recv.at[kind, j], to)

    def all_of(ref, sem):
        pltpu.make_async_copy(ref, ref, sem).wait()

    def w_arrived(kind, j):
        all_of(w1g.at[0 if kind < 3 else 1, pl.ds(0, 3 * wid), span[j]], w_recv.at[kind, j])

    def own_w(w, j):
        return pltpu.make_async_copy(w_src(w, j), w_dst(w, 0, j, OWN), lc_w)

    for r in (PAIR, NEAR, DIAG):
        g_copy(r).start()
    for r in (NEAR, DIAG):
        in_copy(0, r).start()
    for j in range(CHUNKS):
        for w in range(3):
            w_copy(3, w, j).start()
    for i in range(2):
        in_copy(i, PAIR).start()
        own_copy(i).start()
    own_g = pltpu.make_async_copy(g_in, gg.at[t], lc_g)
    own_g.start()
    for j in range(CHUNKS):
        for w in range(3):
            w_copy(1, w, j).start()
            own_w(w, j).start()

    def pass_cross(j):
        w_arrived(3, j)
        for w in range(3):
            w_copy(4, w, j).start()
        if j == 0:
            for r in (NEAR, DIAG):
                in_copy(1, r).start()
        for w in range(3):
            w_copy(5, w, j).start()

    pass_cross(0)
    pass_cross(1)
    own_copy(0).wait()
    own_g.wait()
    for r in (PAIR, NEAR, DIAG):
        in_copy(0, r).wait_recv()
    all_of(gg.at[pl.ds(0, 3)], g_recv)
    gain = jnp.concatenate([gg[k] for k in range(4)], axis=1)
    gain_chip = jnp.concatenate([gg[2 * x], gg[2 * x + 1]], axis=1)

    def blocks(n, body, carry=0, lo=0, hi=None):
        def step(k, carry):
            return body(k, pl.ds(pl.multiple_of(k * n, n), n), carry)
        return lax.fori_loop(lo // n, (tok if hi is None else hi) // n, step, carry, unroll=True)

    def ln_rows(k, rows, carry):
        xf = xg[rows, :].astype(F32)
        mu = jnp.sum(xf, axis=1, keepdims=True) * (1.0 / d)
        s = jnp.sum(xf * xf, axis=1, keepdims=True) * (1.0 / d)
        inv = lax.rsqrt(s - mu * mu + LN_EPS)
        xh = (xf - mu) * inv
        xhat[rows, :] = xh
        inv_std[rows, :] = inv
        h[rows, :] = (gain * xh).astype(BF16)
        h_t[:, rows] = h[rows, chip].astype(F32).T.astype(BF16)
        return carry

    def dy_rows(k, rows, carry):
        dy_t[:, rows] = dyg[rows, chip].astype(F32).T.astype(BF16)
        return carry

    def early_act(k, rows, carry):
        hr = h[rows, :]
        u = dot(hr, w1g[1, :, span[0]])
        v = dot(hr, w3g[1, :, span[0]])
        uv[0, rows, :] = u
        uv[1, rows, :] = v
        act[rows, :size[0]] = (u * (1.0 / (1.0 + jnp.exp(-u))) * v).astype(BF16)
        return carry

    def gated(s, j, known=False):
        n = size[j]

        def body(k, rows, carry):
            if known:
                u, v = uv[0, rows, :], uv[1, rows, :]
            else:
                hr = h[rows, :]
                u = dot(hr, w1g[s, :, span[j]])
                v = dot(hr, w3g[s, :, span[j]])
            da = dot_nt(dyg[rows, :], w2g[s, span[j], :])
            sig = 1.0 / (1.0 + jnp.exp(-u))
            swish = u * sig
            if not known:
                act[rows, :n] = (swish * v).astype(BF16)
            du[rows, :n] = (da * v * sig * (1.0 + u * (1.0 - sig))).astype(BF16)
            dv[rows, :n] = (da * swish).astype(BF16)
            return carry
        blocks(ROW_TILE, body)

    EARLY, LATE1, LATE3 = (2, 3, CHUNKS), (0, 1, 0), (1, 2, CHUNKS + 1)
    FIRST = (EARLY, LATE1, LATE3)

    def bands(j, piece):
        lo, hi, slot = piece or (0, 3, j)
        return pl.ds(lo * wid, (hi - lo) * wid), slot

    def pair_copy(s, j, piece=None):
        band, slot = bands(j, piece)
        return remote(part.at[s, 1 - c, band, span[j]], pair_in.at[s, band, span[j]],
                      dw_send, dw_recv.at[s, slot], dev[PAIR])

    def weight_grads(s, j, lo=0, hi=3):
        for k, (left, right) in tuple(enumerate(((h_t, du), (h_t, dv), (dy_t, act))))[lo:hi]:
            full = dot(left[...], right[:, :size[j]])
            for b in range(2):
                part[s, b, k * wid:(k + 1) * wid, span[j]] = full[b * wid:(b + 1) * wid, :]

    def link_copy(j, piece=None):
        band, slot = bands(j, piece)
        return remote(summed.at[band, span[j]], link_in.at[band, span[j]], lk_send, lk_recv.at[slot], cross)

    def send_sums(j, piece=None):
        band, _ = bands(j, piece)
        pair_copy(1, j, piece).wait_recv()
        summed[band, span[j]] = part[1, c, band, span[j]] + pair_in[1, band, span[j]]
        link_copy(j, piece).start()

    def token_sums(s, j, rows):
        n = size[j]
        m = dot(act[rows, :n], w2g[s, span[j], chip])
        dh = dot_nt(du[rows, :n], w1g[s, chip, span[j]]) + dot_nt(dv[rows, :n], w3g[s, chip, span[j]])
        return m, dh

    def to_tokens(s, j, first=False):
        def body(k, rows, carry):
            m, dh = token_sums(s, j, rows)
            if first:
                m_acc[rows, :] = m
                dh_acc[rows, :] = dh
            else:
                m_acc[rows, :] += m
                dh_acc[rows, :] += dh
            return carry
        blocks(ROW_TILE, body)

    def pass_near(kind, j):
        w_arrived(kind, j)
        for w in range(3):
            w_copy(6 if kind == 4 else 2, w, j).start()

    blocks(LN_ROWS, ln_rows)
    own_copy(1).wait()
    in_copy(1, PAIR).wait_recv()
    blocks(LN_ROWS, dy_rows)
    pass_cross(2)
    pass_near(4, 0)
    w_arrived(5, 0)
    w_arrived(6, 0)
    blocks(ROW_TILE, early_act)
    weight_grads(1, 0, 2, 3)
    pair_copy(1, 0, EARLY).start()
    for j in range(3, CHUNKS):
        pass_cross(j)
    for j in range(CHUNKS):
        for w in range(3):
            w_copy(0, w, j).start()
    send_sums(0, EARLY)
    for r in (NEAR, DIAG):
        in_copy(1, r).wait_recv()

    for j in range(CHUNKS):
        if j:
            w_arrived(5, j)
            w_arrived(6, j)
        if j > 1:
            send_sums(j - 1)
        gated(1, j, known=j == 0)
        if j == 0:
            for k, piece in enumerate((LATE1, LATE3)):
                weight_grads(1, j, k, k + 1)
                pair_copy(1, j, piece).start()
        else:
            weight_grads(1, j)
        to_tokens(1, j, first=j == 0)
        if j == 0:
            send_sums(j, LATE1)
            send_sums(j, LATE3)
        else:
            pair_copy(1, j).start()
        if j + 1 < CHUNKS:
            pass_near(4, j + 1)
        else:
            pass_near(0, 0)

    def finish_dw(j):
        pair_copy(0, j).wait_recv()
        for piece in FIRST if j == 0 else (None,):
            link_copy(j, piece).wait_recv()
        for k in range(3):
            band = pl.ds(k * wid, wid)
            total = part[0, c, band, span[j]] + pair_in[0, band, span[j]] + link_in[band, span[j]]
            if k == 2:
                dw2_out[span[j], :] = total.T
            else:
                (dw1_out, dw3_out)[k][:, span[j]] = total

    lane = lax.broadcasted_iota(jnp.int32, (LN_ROWS, LN_ROWS), 1)
    last = CHUNKS - 1

    def sum_rows(k, rows, carry):
        e = dh_acc[rows, :] * gain_chip
        se = jnp.sum(e, axis=1, keepdims=True)
        sex = jnp.sum(e * xhat[rows, chip], axis=1, keepdims=True)
        st_own[k] = jnp.where(lane == 0, se, jnp.where(lane == 1, sex, 0.0)).T[:8, :]
        return carry

    st_copy = remote(st_own, st_in, st_send, st_recv, dev[NEAR])
    for j in range(CHUNKS):
        w_arrived(1, j)
        w_arrived(2, j)
        if j == 0:
            send_sums(last)
            ref = w1g.at[0, pl.ds(0, 3 * wid), :]
            pltpu.make_async_copy(ref, ref, lc_w).wait()
        gated(0, j)
        weight_grads(0, j)
        if j < last:
            to_tokens(0, j)
            pair_copy(0, j).start()
            if j == last - 1:
                blocks(LN_ROWS, sum_rows)
                st_copy.start()
            pass_near(0, j + 1)
            if j:
                finish_dw(j - 1)
    pair_copy(0, last).start()
    st_copy.wait_recv()

    outs, stage = (y_out, dx_out), (y_st, dx_st)
    mid = tok // 2

    def out_copy(i, part_of):
        rows = pl.ds(part_of * mid, mid)
        to_rows = pl.ds(pl.multiple_of(c * tok + part_of * mid, mid), mid)
        return remote(stage[i].at[rows, core_cols(1 - c)], outs[i].at[to_rows, :],
                      out_send, out_recv, dev[PAIR])

    def out_rows(k):
        return pl.ds(pl.multiple_of(c * tok + k * LN_ROWS, LN_ROWS), LN_ROWS)

    def last_rows(k, rows, dg):
        n = size[last]
        full = dot_nt(du[rows, :n], w1g[0, :, span[last]]) + dot_nt(dv[rows, :n], w3g[0, :, span[last]])
        dh_last[rows, :] = full
        e = full * gain
        before = jnp.concatenate([st_own[k] + st_in[k], jnp.zeros((LN_ROWS - 8, LN_ROWS), F32)], axis=0).T
        means[0, rows, :] = (before[:, 0:1] + jnp.sum(e, axis=1, keepdims=True)) * (1.0 / d)
        means[1, rows, :] = (before[:, 1:2] + jnp.sum(e * xhat[rows, :], axis=1, keepdims=True)) * (1.0 / d)
        dh = dh_acc[rows, :] + dh_last[rows, chip]
        dh_acc[rows, :] = dh
        return dg + jnp.sum(dh * xhat[rows, chip], axis=0, keepdims=True)

    def out_blocks(k, rows, carry):
        dx_ln = inv_std[rows, :] * (dh_acc[rows, :] * gain_chip - means[0, rows, :] - xhat[rows, chip] * means[1, rows, :])
        dx_st[rows, :] = (dyg[rows, chip].astype(F32) + dx_ln).astype(BF16)
        dx_out[out_rows(k), :] = dx_st[rows, core_cols(c)]
        m = dot(act[rows, :size[last]], w2g[0, span[last], chip])
        y_st[rows, :] = (xg[rows, chip].astype(F32) + (m_acc[rows, :] + m)).astype(BF16)
        y_out[out_rows(k), :] = y_st[rows, core_cols(c)]
        return carry

    dg = blocks(LN_ROWS, last_rows, jnp.zeros((1, half), F32))
    for b in range(2):
        dg_st[b] = dg[:, b * wid:(b + 1) * wid]
    for k, (b, to) in enumerate(((1 - c, dev[PAIR]), (c, cross), (1 - c, cross_pair))):
        remote(dg_st.at[b], dg_in.at[k], dg_send, dg_recv, to).start()
    for b in range(2):
        blocks(LN_ROWS, out_blocks, lo=b * mid, hi=(b + 1) * mid)
        out_copy(0, b).start()
        out_copy(1, b).start()

    all_of(gg.at[pl.ds(0, 3)], g_send)
    all_of(part.at[0, 0], in_send)
    all_of(part.at[0], w_send.at[0])
    all_of(part.at[0, :, :, pl.ds(0, 6 * unit)], w_send.at[1])
    all_of(part.at[0], dw_send)
    st_copy.wait_send()
    finish_dw(last - 1)
    finish_dw(last)
    all_of(dg_in, dg_recv)
    dg_out[...] = dg_st[c] + dg_in[0] + dg_in[1] + dg_in[2]
    all_of(dg_in, dg_send)
    all_of(part.at[0, 0], lk_send)
    all_of(dyg.at[pl.ds(0, mid), :], out_send)
    all_of(dyg.at[pl.ds(0, mid), :], out_recv)


def write_out(*refs):
    n = len(refs) // 2
    copies = [pltpu.make_async_copy(refs[i], refs[n + i], refs[2 * n].at[i]) for i in range(n)]
    for cp in copies:
        cp.start()
    for cp in copies:
        cp.wait()


def solution(mesh):
    def local_step(x_blk, dy_blk, gain_blk, w_gate_blk, w_up_blk, w_down_blk):
        rows, wid = x_blk.shape
        f = w_gate_blk.shape[1]
        tok, d, half, fc = rows // 2, 4 * wid, 2 * wid, f // 8 * max(EIGHTHS)
        vm, dma = pltpu.VMEM, pltpu.SemaphoreType.DMA
        in_vmem = pl.BlockSpec(memory_space=pltpu.VMEM)
        args = (x_blk, dy_blk, gain_blk.reshape(1, wid), w_gate_blk, w_up_blk, w_down_blk)
        outs = pl.pallas_call(
            kernel,
            name="mlp_branch",
            out_shape=(jax.ShapeDtypeStruct((rows, wid), BF16), jax.ShapeDtypeStruct((rows, wid), BF16),
                       jax.ShapeDtypeStruct((wid, f), F32), jax.ShapeDtypeStruct((wid, f), F32),
                       jax.ShapeDtypeStruct((f, wid), F32), jax.ShapeDtypeStruct((1, wid), F32)),
            in_specs=[pl.BlockSpec(memory_space=pltpu.HBM)] * 6,
            out_specs=(in_vmem,) * 6,
            scratch_shapes=[
                vm((tok, d), BF16), vm((tok, d), BF16), vm((4, 1, wid), F32),
                vm((2, d, f), BF16), vm((2, d, f), BF16), vm((2, f, d), BF16),
                vm((tok, d), BF16), vm((half, tok), BF16), vm((half, tok), BF16), vm((tok, d), F32), vm((tok, 1), F32),
                vm((2, tok, f // 8 * EIGHTHS[0]), F32),
                vm((tok, fc), BF16), vm((tok, fc), BF16), vm((tok, fc), BF16),
                vm((2, 2, 3 * wid, f), F32), vm((2, 3 * wid, f), F32), vm((3 * wid, f), F32), vm((3 * wid, f), F32),
                vm((tok, half), F32), vm((tok, half), F32), vm((tok, d), F32), vm((2, tok, 1), F32),
                vm((tok, half), BF16), vm((tok, half), BF16),
                vm((2, 1, wid), F32), vm((3, 1, wid), F32),
                vm((tok // LN_ROWS, 8, LN_ROWS), F32), vm((tok // LN_ROWS, 8, LN_ROWS), F32),
                dma(()), dma(()), dma(()), dma((2, 3)),
                dma((2,)), dma((7, CHUNKS)), dma(()), dma((2, CHUNKS + 2)),
                dma(()), dma((CHUNKS + 2,)), dma(()), dma(()), dma(()), dma(()), dma(()), dma(()),
                dma((2,)), dma(()), dma(()),
            ],
            compiler_params=pltpu.CompilerParams(collective_id=0, has_side_effects=True,
                                                 vmem_limit_bytes=44 * 2 ** 20),
        )(*(pltpu.with_memory_space_constraint(a, pltpu.HBM) for a in args))
        outs = pl.pallas_call(
            write_out,
            name="write_out",
            out_shape=tuple(jax.ShapeDtypeStruct(o.shape, o.dtype) for o in outs),
            in_specs=[in_vmem] * 6,
            out_specs=(pl.BlockSpec(memory_space=pl.ANY),) * 6,
            scratch_shapes=[dma((6,))],
            compiler_params=pltpu.CompilerParams(vmem_limit_bytes=2 ** 20),
        )(*outs)
        return outs[:5] + (outs[5].reshape(wid),)

    return jax.shard_map(
        local_step, mesh=mesh,
        in_specs=(P("ty", "tx"), P("ty", "tx"), P("tx"), P("tx", "ty"), P("tx", "ty"), P("ty", "tx")),
        out_specs=(P("ty", "tx"), P("ty", "tx"), P("tx", "ty"), P("tx", "ty"), P("ty", "tx"), P("tx")),
        check_vma=False)
```

```python
import jax
import jax.numpy as jnp
from jax import lax
from jax.experimental import pallas as pl
from jax.experimental.pallas import tpu as pltpu
from jax.sharding import PartitionSpec as P

LN_EPS = 1e-6
MESH = pl.DeviceIdType.MESH
F32 = jnp.float32
BF16 = jnp.bfloat16

OWN, PAIR, NEAR, DIAG = 0, 1, 2, 3
EIGHTHS = (2, 2, 2, 2)
CHUNKS = len(EIGHTHS)
LN_ROWS = 128
ROW_TILE = 256


def dot(a, b):
    return lax.dot_general(a, b, (((1,), (0,)), ((), ())), preferred_element_type=F32)


def dot_nt(a, b):
    return lax.dot_general(a, b, (((1,), (1,)), ((), ())), preferred_element_type=F32)


def kernel(x_in, dy_in, g_in, w1_in, w3_in, w2_in,
           y_out, dx_out, dw1_out, dw3_out, dw2_out, dg_out,
           xg, dyg, gg, w1g, w3g, w2g, h, h_t, dy_t, xhat, inv_std, uv, act, du, dv, part, pair_in, summed, link_in,
           m_acc, dh_acc, dh_last, y_st, dx_st, dg_st, dg_in, st_own, st_in,
           g_send, g_recv, in_send, in_recv, w_send, w_recv, dw_send, dw_recv,
           lk_send, lk_recv, out_send, out_recv, dg_send, dg_recv, st_send, st_recv, lc_in, lc_w, lc_g):
    y, t = lax.axis_index("ty"), lax.axis_index("tx")
    x, c = t // 2, t % 2
    tok = x_in.shape[0] // 2
    wid = x_in.shape[1]
    d = 4 * wid
    half = 2 * wid
    unit = w1_in.shape[1] // 8
    size = [e * unit for e in EIGHTHS]
    start = [sum(size[:i]) for i in range(CHUNKS)]
    span = [pl.ds(start[i], size[i]) for i in range(CHUNKS)]
    peer_t = (t, 2 * x + 1 - c, 2 * (1 - x) + c, 2 * (1 - x) + 1 - c)
    peer_c = (c, 1 - c, c, 1 - c)
    dev = {r: (y, peer_t[r]) for r in (PAIR, NEAR, DIAG)}
    cross, cross_pair = (1 - y, t), (1 - y, peer_t[PAIR])

    barrier = pltpu.get_barrier_semaphore()
    for to in (dev[PAIR], dev[NEAR], dev[DIAG], cross, cross_pair):
        pl.semaphore_signal(barrier, inc=1, device_id=to, device_id_type=MESH)
    pl.semaphore_wait(barrier, 5)

    def remote(src, dst, send, recv, to):
        return pltpu.make_async_remote_copy(src_ref=src, dst_ref=dst, send_sem=send, recv_sem=recv,
                                            device_id=to, device_id_type=MESH)

    def col(r):
        return pl.ds(pl.multiple_of(peer_t[r] * wid, wid), wid)

    def rows_of(core):
        return pl.ds(pl.multiple_of(core * tok, tok), tok)

    def core_cols(core):
        return pl.ds(pl.multiple_of(core * wid, wid), wid)

    chip = pl.ds(pl.multiple_of(x * half, half), half)
    tin, tg = (x_in, dy_in), (xg, dyg)

    def in_copy(i, r):
        return remote(tin[i].at[rows_of(peer_c[r]), :], tg[i].at[:, col(OWN)], in_send, in_recv.at[i, r - 1], dev[r])

    def own_copy(i):
        return pltpu.make_async_copy(tin[i].at[rows_of(c), :], tg[i].at[:, col(OWN)], lc_in.at[i])

    def g_copy(r):
        return remote(g_in, gg.at[t], g_send, g_recv, dev[r])

    def w_src(w, j):
        if w == 2:
            return w2_in.at[span[j], :]
        return (w1_in, w3_in)[w].at[:, span[j]]

    def w_dst(w, side, j, r):
        if w == 2:
            return w2g.at[side, span[j], col(r)]
        return (w1g, w3g)[w].at[side, col(r), span[j]]

    def w_copy(kind, w, j):
        if kind == 0:
            src, dst, to = w_src(w, j), w_dst(w, 0, j, OWN), dev[NEAR]
        elif kind == 1:
            src, dst, to = w_src(w, j), w_dst(w, 0, j, OWN), dev[PAIR]
        elif kind == 2:
            src, dst, to = w_dst(w, 0, j, NEAR), w_dst(w, 0, j, NEAR), dev[PAIR]
        elif kind == 3:
            src, dst, to = w_src(w, j), w_dst(w, 1, j, OWN), cross
        elif kind == 4:
            src, dst, to = w_dst(w, 1, j, OWN), w_dst(w, 1, j, OWN), dev[NEAR]
        elif kind == 5:
            src, dst, to = w_dst(w, 1, j, OWN), w_dst(w, 1, j, OWN), dev[PAIR]
        else:
            src, dst, to = w_dst(w, 1, j, NEAR), w_dst(w, 1, j, NEAR), dev[PAIR]
        slot = CHUNKS if kind in (0, 2) and w == 2 and j == CHUNKS - 1 else j
        return remote(src, dst, w_send.at[kind // 4], w_recv.at[kind, slot], to)

    def all_of(ref, sem):
        pltpu.make_async_copy(ref, ref, sem).wait()

    def w_arrived(kind, j, n=3, slot=None):
        all_of(w1g.at[0 if kind < 3 else 1, pl.ds(0, n * wid), span[j]], w_recv.at[kind, j if slot is None else slot])

    def own_w(w, j):
        return pltpu.make_async_copy(w_src(w, j), w_dst(w, 0, j, OWN), lc_w)

    for r in (PAIR, NEAR, DIAG):
        g_copy(r).start()
    for r in (NEAR, DIAG):
        in_copy(0, r).start()
    for j in range(CHUNKS):
        for w in range(3):
            w_copy(3, w, j).start()
    for i in range(2):
        in_copy(i, PAIR).start()
        own_copy(i).start()
    own_g = pltpu.make_async_copy(g_in, gg.at[t], lc_g)
    own_g.start()
    for j in range(CHUNKS):
        for w in range(3):
            w_copy(1, w, j).start()
            own_w(w, j).start()

    def pass_cross(j):
        w_arrived(3, j)
        for w in range(3):
            w_copy(4, w, j).start()
        if j == 0:
            for r in (NEAR, DIAG):
                in_copy(1, r).start()
        for w in range(3):
            w_copy(5, w, j).start()

    pass_cross(0)
    pass_cross(1)
    own_copy(0).wait()
    own_g.wait()
    for r in (PAIR, NEAR, DIAG):
        in_copy(0, r).wait_recv()
    all_of(gg.at[pl.ds(0, 3)], g_recv)
    gain = jnp.concatenate([gg[k] for k in range(4)], axis=1)
    gain_chip = jnp.concatenate([gg[2 * x], gg[2 * x + 1]], axis=1)

    def blocks(n, body, carry=0, lo=0, hi=None):
        def step(k, carry):
            return body(k, pl.ds(pl.multiple_of(k * n, n), n), carry)
        return lax.fori_loop(lo // n, (tok if hi is None else hi) // n, step, carry, unroll=True)

    def ln_rows(k, rows, carry):
        xf = xg[rows, :].astype(F32)
        mu = jnp.sum(xf, axis=1, keepdims=True) * (1.0 / d)
        s = jnp.sum(xf * xf, axis=1, keepdims=True) * (1.0 / d)
        inv = lax.rsqrt(s - mu * mu + LN_EPS)
        xh = (xf - mu) * inv
        xhat[rows, :] = xh
        inv_std[rows, :] = inv
        h[rows, :] = (gain * xh).astype(BF16)
        h_t[:, rows] = h[rows, chip].astype(F32).T.astype(BF16)
        return carry

    def dy_rows(k, rows, carry):
        dy_t[:, rows] = dyg[rows, chip].astype(F32).T.astype(BF16)
        return carry

    def early_act(s, j):
        def body(k, rows, carry):
            hr = h[rows, :]
            u = dot(hr, w1g[s, :, span[j]])
            v = dot(hr, w3g[s, :, span[j]])
            uv[0, rows, :] = u
            uv[1, rows, :] = v
            act[rows, :size[j]] = (u * (1.0 / (1.0 + jnp.exp(-u))) * v).astype(BF16)
            return carry
        blocks(ROW_TILE, body)

    def gated(s, j, known=False):
        n = size[j]

        def body(k, rows, carry):
            if known:
                u, v = uv[0, rows, :], uv[1, rows, :]
            else:
                hr = h[rows, :]
                u = dot(hr, w1g[s, :, span[j]])
                v = dot(hr, w3g[s, :, span[j]])
            da = dot_nt(dyg[rows, :], w2g[s, span[j], :])
            sig = 1.0 / (1.0 + jnp.exp(-u))
            swish = u * sig
            if not known:
                act[rows, :n] = (swish * v).astype(BF16)
            du[rows, :n] = (da * v * sig * (1.0 + u * (1.0 - sig))).astype(BF16)
            dv[rows, :n] = (da * swish).astype(BF16)
            return carry
        blocks(ROW_TILE, body)

    EARLY, LATE1, LATE3 = (2, 3, CHUNKS), (0, 1, 0), (1, 2, CHUNKS + 1)
    FIRST = (EARLY, LATE1, LATE3)

    def bands(j, piece):
        lo, hi, slot = piece or (0, 3, j)
        return pl.ds(lo * wid, (hi - lo) * wid), slot

    def pair_copy(s, j, piece=None):
        band, slot = bands(j, piece)
        return remote(part.at[s, 1 - c, band, span[j]], pair_in.at[s, band, span[j]],
                      dw_send, dw_recv.at[s, slot], dev[PAIR])

    def weight_grads(s, j, lo=0, hi=3):
        for k, (left, right) in tuple(enumerate(((h_t, du), (h_t, dv), (dy_t, act))))[lo:hi]:
            full = dot(left[...], right[:, :size[j]])
            for b in range(2):
                part[s, b, k * wid:(k + 1) * wid, span[j]] = full[b * wid:(b + 1) * wid, :]

    def link_copy(j, piece=None):
        band, slot = bands(j, piece)
        return remote(summed.at[band, span[j]], link_in.at[band, span[j]], lk_send, lk_recv.at[slot], cross)

    def send_sums(j, piece=None):
        band, _ = bands(j, piece)
        pair_copy(1, j, piece).wait_recv()
        summed[band, span[j]] = part[1, c, band, span[j]] + pair_in[1, band, span[j]]
        link_copy(j, piece).start()

    def token_sums(s, j, rows):
        n = size[j]
        m = dot(act[rows, :n], w2g[s, span[j], chip])
        dh = dot_nt(du[rows, :n], w1g[s, chip, span[j]]) + dot_nt(dv[rows, :n], w3g[s, chip, span[j]])
        return m, dh

    def to_tokens(s, j, first=False):
        def body(k, rows, carry):
            m, dh = token_sums(s, j, rows)
            if first:
                m_acc[rows, :] = m
                dh_acc[rows, :] = dh
            else:
                m_acc[rows, :] += m
                dh_acc[rows, :] += dh
            return carry
        blocks(ROW_TILE, body)

    def pass_near(kind, j):
        n = 2 if kind == 0 and j == CHUNKS - 1 else 3
        w_arrived(kind, j, n)
        for w in range(n):
            w_copy(6 if kind == 4 else 2, w, j).start()

    blocks(LN_ROWS, ln_rows)
    own_copy(1).wait()
    in_copy(1, PAIR).wait_recv()
    blocks(LN_ROWS, dy_rows)
    pass_cross(2)
    pass_near(4, 0)
    w_arrived(5, 0)
    w_arrived(6, 0)
    early_act(1, 0)
    weight_grads(1, 0, 2, 3)
    pair_copy(1, 0, EARLY).start()
    for j in range(3, CHUNKS):
        pass_cross(j)
    for j in range(CHUNKS):
        for w in range(3):
            w_copy(0, w, j).start()
    send_sums(0, EARLY)
    for r in (NEAR, DIAG):
        in_copy(1, r).wait_recv()

    for j in range(CHUNKS):
        if j:
            w_arrived(5, j)
            w_arrived(6, j)
        if j > 2:
            send_sums(j - 1)
        gated(1, j, known=j == 0)
        if j == 0:
            for k, piece in enumerate((LATE1, LATE3)):
                weight_grads(1, j, k, k + 1)
                pair_copy(1, j, piece).start()
        else:
            weight_grads(1, j)
        if j == 1:
            pair_copy(1, j).start()
        if j + 1 == CHUNKS:
            pass_near(0, 0)
        to_tokens(1, j, first=j == 0)
        if j == 0:
            send_sums(j, LATE1)
            send_sums(j, LATE3)
        elif j == 1:
            send_sums(j)
        else:
            pair_copy(1, j).start()
        if j + 1 < CHUNKS:
            pass_near(4, j + 1)

    def finish_dw(j):
        pair_copy(0, j).wait_recv()
        for piece in FIRST if j == 0 else (None,):
            link_copy(j, piece).wait_recv()
        for k in range(3):
            band = pl.ds(k * wid, wid)
            total = part[0, c, band, span[j]] + pair_in[0, band, span[j]] + link_in[band, span[j]]
            if k == 2:
                dw2_out[span[j], :] = total.T
            else:
                (dw1_out, dw3_out)[k][:, span[j]] = total

    lane = lax.broadcasted_iota(jnp.int32, (LN_ROWS, LN_ROWS), 1)
    last = CHUNKS - 1

    def sum_rows(k, rows, carry):
        e = dh_acc[rows, :] * gain_chip
        se = jnp.sum(e, axis=1, keepdims=True)
        sex = jnp.sum(e * xhat[rows, chip], axis=1, keepdims=True)
        st_own[k] = jnp.where(lane == 0, se, jnp.where(lane == 1, sex, 0.0)).T[:8, :]
        return carry

    st_copy = remote(st_own, st_in, st_send, st_recv, dev[NEAR])
    for j in range(CHUNKS):
        w_arrived(1, j)
        w_arrived(2, j, 2 if j == last else 3)
        if j == 0:
            send_sums(last)
            ref = w1g.at[0, pl.ds(0, 3 * wid), :]
            pltpu.make_async_copy(ref, ref, lc_w).wait()
        if j == last:
            early_act(0, j)
            weight_grads(0, j, 2, 3)
            w_arrived(2, j, 1, CHUNKS)
        gated(0, j, known=j == last)
        weight_grads(0, j, 0, 2 if j == last else 3)
        if j < last:
            if j != last - 2:
                pass_near(0, j + 1)
            to_tokens(0, j)
            pair_copy(0, j).start()
            if j == last - 2:
                pass_near(0, j + 1)
            if j == last - 1:
                blocks(LN_ROWS, sum_rows)
                st_copy.start()
                w_arrived(0, last, 1, CHUNKS)
                w_copy(2, 2, last).start()
            if j:
                finish_dw(j - 1)
    pair_copy(0, last).start()

    outs, stage = (y_out, dx_out), (y_st, dx_st)
    mid = tok // 2

    def out_copy(i, part_of):
        rows = pl.ds(part_of * mid, mid)
        to_rows = pl.ds(pl.multiple_of(c * tok + part_of * mid, mid), mid)
        return remote(stage[i].at[rows, core_cols(1 - c)], outs[i].at[to_rows, :],
                      out_send, out_recv, dev[PAIR])

    def out_rows(k):
        return pl.ds(pl.multiple_of(c * tok + k * LN_ROWS, LN_ROWS), LN_ROWS)

    def last_rows(k, rows, dg):
        n = size[last]
        dh_last[rows, :] = dot_nt(du[rows, :n], w1g[0, :, span[last]]) + dot_nt(dv[rows, :n], w3g[0, :, span[last]])
        dh = dh_acc[rows, :] + dh_last[rows, chip]
        dh_acc[rows, :] = dh
        return dg + jnp.sum(dh * xhat[rows, chip], axis=0, keepdims=True)

    def out_blocks(k, rows, carry):
        e = dh_last[rows, :] * gain
        before = jnp.concatenate([st_own[k] + st_in[k], jnp.zeros((LN_ROWS - 8, LN_ROWS), F32)], axis=0).T
        me = (before[:, 0:1] + jnp.sum(e, axis=1, keepdims=True)) * (1.0 / d)
        mex = (before[:, 1:2] + jnp.sum(e * xhat[rows, :], axis=1, keepdims=True)) * (1.0 / d)
        dx_ln = inv_std[rows, :] * (dh_acc[rows, :] * gain_chip - me - xhat[rows, chip] * mex)
        dx_st[rows, :] = (dyg[rows, chip].astype(F32) + dx_ln).astype(BF16)
        dx_out[out_rows(k), :] = dx_st[rows, core_cols(c)]
        m = dot(act[rows, :size[last]], w2g[0, span[last], chip])
        y_st[rows, :] = (xg[rows, chip].astype(F32) + (m_acc[rows, :] + m)).astype(BF16)
        y_out[out_rows(k), :] = y_st[rows, core_cols(c)]
        return carry

    dg = blocks(LN_ROWS, last_rows, jnp.zeros((1, half), F32))
    for b in range(2):
        dg_st[b] = dg[:, b * wid:(b + 1) * wid]
    for k, (b, to) in enumerate(((1 - c, dev[PAIR]), (c, cross), (1 - c, cross_pair))):
        remote(dg_st.at[b], dg_in.at[k], dg_send, dg_recv, to).start()
    st_copy.wait_recv()
    for b in range(2):
        blocks(LN_ROWS, out_blocks, lo=b * mid, hi=(b + 1) * mid)
        out_copy(0, b).start()
        out_copy(1, b).start()

    all_of(gg.at[pl.ds(0, 3)], g_send)
    all_of(part.at[0, 0], in_send)
    all_of(part.at[0], w_send.at[0])
    all_of(part.at[0, :, :, pl.ds(0, 6 * unit)], w_send.at[1])
    all_of(part.at[0], dw_send)
    st_copy.wait_send()
    finish_dw(last - 1)
    finish_dw(last)
    all_of(dg_in, dg_recv)
    dg_out[...] = dg_st[c] + dg_in[0] + dg_in[1] + dg_in[2]
    all_of(dg_in, dg_send)
    all_of(part.at[0, 0], lk_send)
    all_of(dyg.at[pl.ds(0, mid), :], out_send)
    all_of(dyg.at[pl.ds(0, mid), :], out_recv)


def write_out(*refs):
    n = len(refs) // 2
    copies = [pltpu.make_async_copy(refs[i], refs[n + i], refs[2 * n].at[i]) for i in range(n)]
    for cp in copies:
        cp.start()
    for cp in copies:
        cp.wait()


def solution(mesh):
    def local_step(x_blk, dy_blk, gain_blk, w_gate_blk, w_up_blk, w_down_blk):
        rows, wid = x_blk.shape
        f = w_gate_blk.shape[1]
        tok, d, half, fc = rows // 2, 4 * wid, 2 * wid, f // 8 * max(EIGHTHS)
        vm, dma = pltpu.VMEM, pltpu.SemaphoreType.DMA
        in_vmem = pl.BlockSpec(memory_space=pltpu.VMEM)
        args = (x_blk, dy_blk, gain_blk.reshape(1, wid), w_gate_blk, w_up_blk, w_down_blk)
        outs = pl.pallas_call(
            kernel,
            name="mlp_branch",
            out_shape=(jax.ShapeDtypeStruct((rows, wid), BF16), jax.ShapeDtypeStruct((rows, wid), BF16),
                       jax.ShapeDtypeStruct((wid, f), F32), jax.ShapeDtypeStruct((wid, f), F32),
                       jax.ShapeDtypeStruct((f, wid), F32), jax.ShapeDtypeStruct((1, wid), F32)),
            in_specs=[pl.BlockSpec(memory_space=pltpu.HBM)] * 6,
            out_specs=(in_vmem,) * 6,
            scratch_shapes=[
                vm((tok, d), BF16), vm((tok, d), BF16), vm((4, 1, wid), F32),
                vm((2, d, f), BF16), vm((2, d, f), BF16), vm((2, f, d), BF16),
                vm((tok, d), BF16), vm((half, tok), BF16), vm((half, tok), BF16), vm((tok, d), F32), vm((tok, 1), F32),
                vm((2, tok, f // 8 * EIGHTHS[0]), F32),
                vm((tok, fc), BF16), vm((tok, fc), BF16), vm((tok, fc), BF16),
                vm((2, 2, 3 * wid, f), F32), vm((2, 3 * wid, f), F32), vm((3 * wid, f), F32), vm((3 * wid, f), F32),
                vm((tok, half), F32), vm((tok, half), F32), vm((tok, d), F32),
                vm((tok, half), BF16), vm((tok, half), BF16),
                vm((2, 1, wid), F32), vm((3, 1, wid), F32),
                vm((tok // LN_ROWS, 8, LN_ROWS), F32), vm((tok // LN_ROWS, 8, LN_ROWS), F32),
                dma(()), dma(()), dma(()), dma((2, 3)),
                dma((2,)), dma((7, CHUNKS + 1)), dma(()), dma((2, CHUNKS + 2)),
                dma(()), dma((CHUNKS + 2,)), dma(()), dma(()), dma(()), dma(()), dma(()), dma(()),
                dma((2,)), dma(()), dma(()),
            ],
            compiler_params=pltpu.CompilerParams(collective_id=0, has_side_effects=True,
                                                 vmem_limit_bytes=44 * 2 ** 20),
        )(*(pltpu.with_memory_space_constraint(a, pltpu.HBM) for a in args))
        outs = pl.pallas_call(
            write_out,
            name="write_out",
            out_shape=tuple(jax.ShapeDtypeStruct(o.shape, o.dtype) for o in outs),
            in_specs=[in_vmem] * 6,
            out_specs=(pl.BlockSpec(memory_space=pl.ANY),) * 6,
            scratch_shapes=[dma((6,))],
            compiler_params=pltpu.CompilerParams(vmem_limit_bytes=2 ** 20),
        )(*outs)
        return outs[:5] + (outs[5].reshape(wid),)

    return jax.shard_map(
        local_step, mesh=mesh,
        in_specs=(P("ty", "tx"), P("ty", "tx"), P("tx"), P("tx", "ty"), P("tx", "ty"), P("ty", "tx")),
        out_specs=(P("ty", "tx"), P("ty", "tx"), P("tx", "ty"), P("tx", "ty"), P("ty", "tx"), P("tx")),
        check_vma=False)
```

```python
import jax
import jax.numpy as jnp
from jax import lax
from jax.experimental import pallas as pl
from jax.experimental.pallas import tpu as pltpu
from jax.sharding import PartitionSpec as P

LN_EPS = 1e-6
MESH = pl.DeviceIdType.MESH
F32 = jnp.float32
BF16 = jnp.bfloat16

OWN, PAIR, NEAR, DIAG = 0, 1, 2, 3
EIGHTHS = (2, 2, 2, 2)
CHUNKS = len(EIGHTHS)
LN_ROWS = 128
ROW_TILE = 256
PIECES = 4


def dot(a, b):
    return lax.dot_general(a, b, (((1,), (0,)), ((), ())), preferred_element_type=F32)


def dot_nt(a, b):
    return lax.dot_general(a, b, (((1,), (1,)), ((), ())), preferred_element_type=F32)


def kernel(x_in, dy_in, g_in, w1_in, w3_in, w2_in,
           y_out, dx_out, dw1_out, dw3_out, dw2_out, dg_out,
           xg, dyg, gg, w1g, w3g, w2g, h, h_t, dy_t, xhat, inv_std, uv, act, du, dv, part, pair_in, summed, link_in,
           m_acc, dh_acc, dh_last, y_st, dx_st, dg_st, dg_in, st_own, st_in,
           g_send, g_recv, in_send, in_recv, w_send, w_recv, dw_send, dw_recv,
           lk_send, lk_recv, out_send, out_recv, dg_send, dg_recv, st_send, st_recv, lc_in, lc_w, lc_g):
    y, t = lax.axis_index("ty"), lax.axis_index("tx")
    x, c = t // 2, t % 2
    tok = x_in.shape[0] // 2
    wid = x_in.shape[1]
    d = 4 * wid
    half = 2 * wid
    unit = w1_in.shape[1] // 8
    size = [e * unit for e in EIGHTHS]
    start = [sum(size[:i]) for i in range(CHUNKS)]
    span = [pl.ds(start[i], size[i]) for i in range(CHUNKS)]
    peer_t = (t, 2 * x + 1 - c, 2 * (1 - x) + c, 2 * (1 - x) + 1 - c)
    peer_c = (c, 1 - c, c, 1 - c)
    dev = {r: (y, peer_t[r]) for r in (PAIR, NEAR, DIAG)}
    cross, cross_pair = (1 - y, t), (1 - y, peer_t[PAIR])

    barrier = pltpu.get_barrier_semaphore()
    for to in (dev[PAIR], dev[NEAR], dev[DIAG], cross, cross_pair):
        pl.semaphore_signal(barrier, inc=1, device_id=to, device_id_type=MESH)
    pl.semaphore_wait(barrier, 5)

    def remote(src, dst, send, recv, to):
        return pltpu.make_async_remote_copy(src_ref=src, dst_ref=dst, send_sem=send, recv_sem=recv,
                                            device_id=to, device_id_type=MESH)

    def col(r):
        return pl.ds(pl.multiple_of(peer_t[r] * wid, wid), wid)

    def rows_of(core):
        return pl.ds(pl.multiple_of(core * tok, tok), tok)

    def core_cols(core):
        return pl.ds(pl.multiple_of(core * wid, wid), wid)

    chip = pl.ds(pl.multiple_of(x * half, half), half)
    tin, tg = (x_in, dy_in), (xg, dyg)

    def in_copy(i, r):
        return remote(tin[i].at[rows_of(peer_c[r]), :], tg[i].at[:, col(OWN)], in_send, in_recv.at[i, r - 1], dev[r])

    def own_copy(i):
        return pltpu.make_async_copy(tin[i].at[rows_of(c), :], tg[i].at[:, col(OWN)], lc_in.at[i])

    def g_copy(r):
        return remote(g_in, gg.at[t], g_send, g_recv, dev[r])

    def w_src(w, j):
        if w == 2:
            return w2_in.at[span[j], :]
        return (w1_in, w3_in)[w].at[:, span[j]]

    def w_dst(w, side, j, r):
        if w == 2:
            return w2g.at[side, span[j], col(r)]
        return (w1g, w3g)[w].at[side, col(r), span[j]]

    def w_copy(kind, w, j):
        if kind == 0:
            src, dst, to = w_src(w, j), w_dst(w, 0, j, OWN), dev[NEAR]
        elif kind == 1:
            src, dst, to = w_src(w, j), w_dst(w, 0, j, OWN), dev[PAIR]
        elif kind == 2:
            src, dst, to = w_dst(w, 0, j, NEAR), w_dst(w, 0, j, NEAR), dev[PAIR]
        elif kind == 3:
            src, dst, to = w_src(w, j), w_dst(w, 1, j, OWN), cross
        elif kind == 4:
            src, dst, to = w_dst(w, 1, j, OWN), w_dst(w, 1, j, OWN), dev[NEAR]
        elif kind == 5:
            src, dst, to = w_dst(w, 1, j, OWN), w_dst(w, 1, j, OWN), dev[PAIR]
        else:
            src, dst, to = w_dst(w, 1, j, NEAR), w_dst(w, 1, j, NEAR), dev[PAIR]
        slot = CHUNKS if kind in (0, 2) and w == 2 and j == CHUNKS - 1 else j
        return remote(src, dst, w_send.at[kind // 4], w_recv.at[kind, slot], to)

    def all_of(ref, sem):
        pltpu.make_async_copy(ref, ref, sem).wait()

    def w_arrived(kind, j, n=3, slot=None):
        all_of(w1g.at[0 if kind < 3 else 1, pl.ds(0, n * wid), span[j]], w_recv.at[kind, j if slot is None else slot])

    def own_w(w, j):
        return pltpu.make_async_copy(w_src(w, j), w_dst(w, 0, j, OWN), lc_w)

    for r in (PAIR, NEAR, DIAG):
        g_copy(r).start()
    for r in (NEAR, DIAG):
        in_copy(0, r).start()
    for j in range(CHUNKS):
        for w in range(3):
            w_copy(3, w, j).start()
    for i in range(2):
        in_copy(i, PAIR).start()
        own_copy(i).start()
    own_g = pltpu.make_async_copy(g_in, gg.at[t], lc_g)
    own_g.start()
    for j in range(CHUNKS):
        for w in range(3):
            w_copy(1, w, j).start()
            own_w(w, j).start()

    def pass_cross(j):
        w_arrived(3, j)
        for w in range(3):
            w_copy(4, w, j).start()
        if j == 0:
            for r in (NEAR, DIAG):
                in_copy(1, r).start()
        for w in range(3):
            w_copy(5, w, j).start()

    pass_cross(0)
    pass_cross(1)
    own_copy(0).wait()
    own_g.wait()
    for r in (PAIR, NEAR, DIAG):
        in_copy(0, r).wait_recv()
    all_of(gg.at[pl.ds(0, 3)], g_recv)
    gain = jnp.concatenate([gg[k] for k in range(4)], axis=1)
    gain_chip = jnp.concatenate([gg[2 * x], gg[2 * x + 1]], axis=1)

    def blocks(n, body, carry=0, lo=0, hi=None):
        def step(k, carry):
            return body(k, pl.ds(pl.multiple_of(k * n, n), n), carry)
        return lax.fori_loop(lo // n, (tok if hi is None else hi) // n, step, carry, unroll=True)

    def ln_rows(k, rows, carry):
        xf = xg[rows, :].astype(F32)
        mu = jnp.sum(xf, axis=1, keepdims=True) * (1.0 / d)
        s = jnp.sum(xf * xf, axis=1, keepdims=True) * (1.0 / d)
        inv = lax.rsqrt(s - mu * mu + LN_EPS)
        xh = (xf - mu) * inv
        xhat[rows, :] = xh
        inv_std[rows, :] = inv
        h[rows, :] = (gain * xh).astype(BF16)
        h_t[:, rows] = h[rows, chip].astype(F32).T.astype(BF16)
        return carry

    def dy_rows(k, rows, carry):
        dy_t[:, rows] = dyg[rows, chip].astype(F32).T.astype(BF16)
        return carry

    def early_act(s, j):
        def body(k, rows, carry):
            hr = h[rows, :]
            u = dot(hr, w1g[s, :, span[j]])
            v = dot(hr, w3g[s, :, span[j]])
            uv[0, rows, :] = u
            uv[1, rows, :] = v
            act[rows, :size[j]] = (u * (1.0 / (1.0 + jnp.exp(-u))) * v).astype(BF16)
            return carry
        blocks(ROW_TILE, body)

    def gated(s, j, known=False):
        n = size[j]

        def body(k, rows, carry):
            if known:
                u, v = uv[0, rows, :], uv[1, rows, :]
            else:
                hr = h[rows, :]
                u = dot(hr, w1g[s, :, span[j]])
                v = dot(hr, w3g[s, :, span[j]])
            da = dot_nt(dyg[rows, :], w2g[s, span[j], :])
            sig = 1.0 / (1.0 + jnp.exp(-u))
            swish = u * sig
            if not known:
                act[rows, :n] = (swish * v).astype(BF16)
            du[rows, :n] = (da * v * sig * (1.0 + u * (1.0 - sig))).astype(BF16)
            dv[rows, :n] = (da * swish).astype(BF16)
            return carry
        blocks(ROW_TILE, body)

    EARLY, LATE1, LATE3 = (2, 3, CHUNKS), (0, 1, 0), (1, 2, CHUNKS + 1)
    FIRST = (EARLY, LATE1, LATE3)

    def bands(j, piece):
        lo, hi, slot = piece or (0, 3, j)
        return pl.ds(lo * wid, (hi - lo) * wid), slot

    def pair_copy(s, j, piece=None):
        band, slot = bands(j, piece)
        return remote(part.at[s, 1 - c, band, span[j]], pair_in.at[s, band, span[j]],
                      dw_send, dw_recv.at[s, slot], dev[PAIR])

    def weight_grads(s, j, lo=0, hi=3):
        for k, (left, right) in tuple(enumerate(((h_t, du), (h_t, dv), (dy_t, act))))[lo:hi]:
            full = dot(left[...], right[:, :size[j]])
            for b in range(2):
                part[s, b, k * wid:(k + 1) * wid, span[j]] = full[b * wid:(b + 1) * wid, :]

    def link_copy(j, piece=None):
        band, slot = bands(j, piece)
        return remote(summed.at[band, span[j]], link_in.at[band, span[j]], lk_send, lk_recv.at[slot], cross)

    def send_sums(j, piece=None):
        band, _ = bands(j, piece)
        pair_copy(1, j, piece).wait_recv()
        summed[band, span[j]] = part[1, c, band, span[j]] + pair_in[1, band, span[j]]
        link_copy(j, piece).start()

    def token_sums(s, j, rows):
        n = size[j]
        m = dot(act[rows, :n], w2g[s, span[j], chip])
        dh = dot_nt(du[rows, :n], w1g[s, chip, span[j]]) + dot_nt(dv[rows, :n], w3g[s, chip, span[j]])
        return m, dh

    def to_tokens(s, j, first=False):
        def body(k, rows, carry):
            m, dh = token_sums(s, j, rows)
            if first:
                m_acc[rows, :] = m
                dh_acc[rows, :] = dh
            else:
                m_acc[rows, :] += m
                dh_acc[rows, :] += dh
            return carry
        blocks(ROW_TILE, body)

    def pass_near(kind, j):
        n = 2 if kind == 0 and j == CHUNKS - 1 else 3
        w_arrived(kind, j, n)
        for w in range(n):
            w_copy(6 if kind == 4 else 2, w, j).start()

    blocks(LN_ROWS, ln_rows)
    own_copy(1).wait()
    in_copy(1, PAIR).wait_recv()
    blocks(LN_ROWS, dy_rows)
    pass_cross(2)
    pass_near(4, 0)
    w_arrived(5, 0)
    w_arrived(6, 0)
    early_act(1, 0)
    weight_grads(1, 0, 2, 3)
    pair_copy(1, 0, EARLY).start()
    for j in range(3, CHUNKS):
        pass_cross(j)
    for j in range(CHUNKS):
        for w in range(3):
            w_copy(0, w, j).start()
    send_sums(0, EARLY)
    for r in (NEAR, DIAG):
        in_copy(1, r).wait_recv()

    for j in range(CHUNKS):
        if j:
            w_arrived(5, j)
            w_arrived(6, j)
        if j > 2:
            send_sums(j - 1)
        gated(1, j, known=j == 0)
        if j == 0:
            for k, piece in enumerate((LATE1, LATE3)):
                weight_grads(1, j, k, k + 1)
                pair_copy(1, j, piece).start()
        else:
            weight_grads(1, j)
        if j == 1:
            pair_copy(1, j).start()
        if j + 1 == CHUNKS:
            pass_near(0, 0)
        to_tokens(1, j, first=j == 0)
        if j == 0:
            send_sums(j, LATE1)
            send_sums(j, LATE3)
        elif j == 1:
            send_sums(j)
        else:
            pair_copy(1, j).start()
        if j + 1 < CHUNKS:
            pass_near(4, j + 1)

    def finish_dw(j):
        pair_copy(0, j).wait_recv()
        for piece in FIRST if j == 0 else (None,):
            link_copy(j, piece).wait_recv()
        for k in range(3):
            band = pl.ds(k * wid, wid)
            total = part[0, c, band, span[j]] + pair_in[0, band, span[j]] + link_in[band, span[j]]
            if k == 2:
                dw2_out[span[j], :] = total.T
            else:
                (dw1_out, dw3_out)[k][:, span[j]] = total

    lane = lax.broadcasted_iota(jnp.int32, (LN_ROWS, LN_ROWS), 1)
    last = CHUNKS - 1

    def sum_rows(k, rows, carry):
        e = dh_acc[rows, :] * gain_chip
        se = jnp.sum(e, axis=1, keepdims=True)
        sex = jnp.sum(e * xhat[rows, chip], axis=1, keepdims=True)
        st_own[k] = jnp.where(lane == 0, se, jnp.where(lane == 1, sex, 0.0)).T[:8, :]
        return carry

    st_copy = remote(st_own, st_in, st_send, st_recv, dev[NEAR])
    for j in range(CHUNKS):
        w_arrived(1, j)
        w_arrived(2, j, 2 if j == last else 3)
        if j == 0:
            send_sums(last)
            ref = w1g.at[0, pl.ds(0, 3 * wid), :]
            pltpu.make_async_copy(ref, ref, lc_w).wait()
        if j == last:
            early_act(0, j)
            weight_grads(0, j, 2, 3)
            w_arrived(2, j, 1, CHUNKS)
        gated(0, j, known=j == last)
        weight_grads(0, j, 0, 2 if j == last else 3)
        if j < last:
            if j != last - 2:
                pass_near(0, j + 1)
            to_tokens(0, j)
            pair_copy(0, j).start()
            if j == last - 2:
                pass_near(0, j + 1)
            if j == last - 1:
                blocks(LN_ROWS, sum_rows)
                st_copy.start()
                w_arrived(0, last, 1, CHUNKS)
                w_copy(2, 2, last).start()
            if j:
                finish_dw(j - 1)
    pair_copy(0, last).start()

    outs, stage = (y_out, dx_out), (y_st, dx_st)
    mid = tok // 2

    def out_copy(i, part_of):
        rows = pl.ds(part_of * mid, mid)
        to_rows = pl.ds(pl.multiple_of(c * tok + part_of * mid, mid), mid)
        return remote(stage[i].at[rows, core_cols(1 - c)], outs[i].at[to_rows, :],
                      out_send, out_recv, dev[PAIR])

    def out_rows(k):
        return pl.ds(pl.multiple_of(c * tok + k * LN_ROWS, LN_ROWS), LN_ROWS)

    def last_rows(k, rows, dg):
        n = size[last]
        dh_last[rows, :] = dot_nt(du[rows, :n], w1g[0, :, span[last]]) + dot_nt(dv[rows, :n], w3g[0, :, span[last]])
        dh = dh_acc[rows, :] + dh_last[rows, chip]
        dh_acc[rows, :] = dh
        return dg + jnp.sum(dh * xhat[rows, chip], axis=0, keepdims=True)

    def out_blocks(k, rows, carry):
        e = dh_last[rows, :] * gain
        before = jnp.concatenate([st_own[k] + st_in[k], jnp.zeros((LN_ROWS - 8, LN_ROWS), F32)], axis=0).T
        me = (before[:, 0:1] + jnp.sum(e, axis=1, keepdims=True)) * (1.0 / d)
        mex = (before[:, 1:2] + jnp.sum(e * xhat[rows, :], axis=1, keepdims=True)) * (1.0 / d)
        dx_ln = inv_std[rows, :] * (dh_acc[rows, :] * gain_chip - me - xhat[rows, chip] * mex)
        dx_st[rows, :] = (dyg[rows, chip].astype(F32) + dx_ln).astype(BF16)
        dx_out[out_rows(k), :] = dx_st[rows, core_cols(c)]
        m = dot(act[rows, :size[last]], w2g[0, span[last], chip])
        y_st[rows, :] = (xg[rows, chip].astype(F32) + (m_acc[rows, :] + m)).astype(BF16)
        y_out[out_rows(k), :] = y_st[rows, core_cols(c)]
        return carry

    dg = blocks(LN_ROWS, last_rows, jnp.zeros((1, half), F32))
    for b in range(2):
        dg_st[b] = dg[:, b * wid:(b + 1) * wid]
    for k, (b, to) in enumerate(((1 - c, dev[PAIR]), (c, cross), (1 - c, cross_pair))):
        remote(dg_st.at[b], dg_in.at[k], dg_send, dg_recv, to).start()
    st_copy.wait_recv()
    for b in range(2):
        blocks(LN_ROWS, out_blocks, lo=b * mid, hi=(b + 1) * mid)
        out_copy(0, b).start()
        out_copy(1, b).start()

    all_of(gg.at[pl.ds(0, 3)], g_send)
    all_of(part.at[0, 0], in_send)
    all_of(part.at[0], w_send.at[0])
    all_of(part.at[0, :, :, pl.ds(0, 6 * unit)], w_send.at[1])
    all_of(part.at[0], dw_send)
    st_copy.wait_send()
    finish_dw(last - 1)
    finish_dw(last)
    all_of(dg_in, dg_recv)
    dg_out[...] = dg_st[c] + dg_in[0] + dg_in[1] + dg_in[2]
    all_of(dg_in, dg_send)
    all_of(part.at[0, 0], lk_send)
    all_of(dyg.at[pl.ds(0, mid), :], out_send)
    all_of(dyg.at[pl.ds(0, mid), :], out_recv)


def write_out(*refs):
    n = len(refs) // 2
    copies = []
    for i in range(n):
        rows = refs[i].shape[0]
        pieces = PIECES if rows > PIECES else 1
        for k in range(pieces):
            at = pl.ds(k * (rows // pieces), rows // pieces)
            copies.append(pltpu.make_async_copy(refs[i].at[at, :], refs[n + i].at[at, :], refs[2 * n].at[i, k]))
    for cp in copies:
        cp.start()
    for cp in copies:
        cp.wait()


def solution(mesh):
    def local_step(x_blk, dy_blk, gain_blk, w_gate_blk, w_up_blk, w_down_blk):
        rows, wid = x_blk.shape
        f = w_gate_blk.shape[1]
        tok, d, half, fc = rows // 2, 4 * wid, 2 * wid, f // 8 * max(EIGHTHS)
        vm, dma = pltpu.VMEM, pltpu.SemaphoreType.DMA
        in_vmem = pl.BlockSpec(memory_space=pltpu.VMEM)
        args = (x_blk, dy_blk, gain_blk.reshape(1, wid), w_gate_blk, w_up_blk, w_down_blk)
        outs = pl.pallas_call(
            kernel,
            name="mlp_branch",
            out_shape=(jax.ShapeDtypeStruct((rows, wid), BF16), jax.ShapeDtypeStruct((rows, wid), BF16),
                       jax.ShapeDtypeStruct((wid, f), F32), jax.ShapeDtypeStruct((wid, f), F32),
                       jax.ShapeDtypeStruct((f, wid), F32), jax.ShapeDtypeStruct((1, wid), F32)),
            in_specs=[pl.BlockSpec(memory_space=pltpu.HBM)] * 6,
            out_specs=(in_vmem,) * 6,
            scratch_shapes=[
                vm((tok, d), BF16), vm((tok, d), BF16), vm((4, 1, wid), F32),
                vm((2, d, f), BF16), vm((2, d, f), BF16), vm((2, f, d), BF16),
                vm((tok, d), BF16), vm((half, tok), BF16), vm((half, tok), BF16), vm((tok, d), F32), vm((tok, 1), F32),
                vm((2, tok, f // 8 * EIGHTHS[0]), F32),
                vm((tok, fc), BF16), vm((tok, fc), BF16), vm((tok, fc), BF16),
                vm((2, 2, 3 * wid, f), F32), vm((2, 3 * wid, f), F32), vm((3 * wid, f), F32), vm((3 * wid, f), F32),
                vm((tok, half), F32), vm((tok, half), F32), vm((tok, d), F32),
                vm((tok, half), BF16), vm((tok, half), BF16),
                vm((2, 1, wid), F32), vm((3, 1, wid), F32),
                vm((tok // LN_ROWS, 8, LN_ROWS), F32), vm((tok // LN_ROWS, 8, LN_ROWS), F32),
                dma(()), dma(()), dma(()), dma((2, 3)),
                dma((2,)), dma((7, CHUNKS + 1)), dma(()), dma((2, CHUNKS + 2)),
                dma(()), dma((CHUNKS + 2,)), dma(()), dma(()), dma(()), dma(()), dma(()), dma(()),
                dma((2,)), dma(()), dma(()),
            ],
            compiler_params=pltpu.CompilerParams(collective_id=0, has_side_effects=True,
                                                 vmem_limit_bytes=44 * 2 ** 20),
        )(*(pltpu.with_memory_space_constraint(a, pltpu.HBM) for a in args))
        outs = pl.pallas_call(
            write_out,
            name="write_out",
            out_shape=tuple(jax.ShapeDtypeStruct(o.shape, o.dtype) for o in outs),
            in_specs=[in_vmem] * 6,
            out_specs=(pl.BlockSpec(memory_space=pl.ANY),) * 6,
            scratch_shapes=[dma((6, PIECES))],
            compiler_params=pltpu.CompilerParams(vmem_limit_bytes=2 ** 20),
        )(*outs)
        return outs[:5] + (outs[5].reshape(wid),)

    return jax.shard_map(
        local_step, mesh=mesh,
        in_specs=(P("ty", "tx"), P("ty", "tx"), P("tx"), P("tx", "ty"), P("tx", "ty"), P("ty", "tx")),
        out_specs=(P("ty", "tx"), P("ty", "tx"), P("tx", "ty"), P("tx", "ty"), P("ty", "tx"), P("tx")),
        check_vma=False)
```
